512 devices in a mesh: clump: 128 (over z, y, core), grp: 4 (over x).
Axes of the slice: x: 4, y: 4, z: 16, core: 2. Of those that a mesh axis runs over, the one named last changes fastest.
Arguments:
- flux: float32 [512, 1024, 64], P(('clump', 'grp')), may hold values from -6 to 6
- patch_pft: int32 [512, 1024], P(('clump', 'grp')), may hold values from 0 to 15
- patch_wt: float32 [512, 1024], P(('clump', 'grp')), may hold values from 0.2 to 2
- patch_col: int32 [512, 1024], P(('clump', 'grp')), may hold values from 0 to 511, never falling along the last dimension, each value on 1 to 4 neighbouring positions
- col_wt: float32 [512, 512], P(('clump', 'grp')), may hold values from 0.2 to 2
- col_lu: int32 [512, 512], P(('clump', 'grp')), may hold values from 0 to 255, never falling along the last dimension, each value on 1 to 4 neighbouring positions
- lu_wt: float32 [512, 256], P(('clump', 'grp')), may hold values from 0.2 to 2
- lu_grid: int32 [512, 256], P(('clump', 'grp')), may hold values from 0 to 127, never falling along the last dimension, each value on 1 to 4 neighbouring positions
- cell_target: int32 [512, 128], P(('clump', 'grp')), may hold values from 0 to 65535, as said below
- patch_count: int32 [512], P(('clump', 'grp')), may hold values from 64 to 1024
- pft_scale: float32 [16, 64], replicated, may hold values from 0.3 to 3
- cpl_frac: float32 [65536], P(('clump', 'grp')), may hold values from 0.2 to 0.9
- cpl_field: float32 [65536, 64], P(('clump', 'grp')), may hold values from -6 to 6
Outputs:
- grid_merged: float32 [65536, 64], P(('clump', 'grp'))
- anomaly: float32 [512, 1024, 64], P(('clump', 'grp'))
The draws below stay inside these ranges and needn't reach their ends.
Inputs may be any that keep to these rules, and one draw needn't show every extreme that they name: `patch_col`: within each device's row the column numbers never fall, and each column holds 1 to 4 patch slots. `col_lu`: within each device's row the landunit numbers never fall, and each landunit holds 1 to 4 columns. `lu_grid`: within each device's row the gridcell numbers never fall, and each gridcell holds 1 to 4 landunits. `cell_target`: all devices' entries together are a permutation of 0 to 65535; the coupler owner of an entry q is q // 128, and each device's 128 gridcells go to 64 owners, exactly 2 to each.
All inputs are finite; a program needn't handle non-finite values.
Results may differ from the reference program's by a relative error of at most 0.0003.
Values sent between devices are 32-bit elements; how exact they have to be, the bound alone decides.
No kernel may reach another device: no remote copies, remote signals or barrier semaphores. Data moves between devices by JAX's collectives and lax.ppermute only.
A program may use at most 64 MiB of HBM per device.

```python
import math
import jax
import jax.numpy as jnp
import numpy as np
from jax import lax

NV = 64
NPFT = 16
P_DEV = 1024
C_DEV = 512
L_DEV = 256
G_DEV = 128
CAP = 2
GRID = 65536
DEVICES = 512


def row_orders(key, rows, length):

    def single(row_key):
        return jax.random.permutation(row_key, length)
    return jax.vmap(single)(jax.random.split(key, rows))


def draw_cell_target(key, part):
    key_shift, key_label, key_local, key_slot = jax.random.split(jax.random.fold_in(key, 11), 4)
    shift = jax.random.permutation(key_shift, DEVICES).astype(jnp.int32)
    label = jax.random.permutation(key_label, DEVICES).astype(jnp.int32)
    local_order = row_orders(key_local, DEVICES, G_DEV).astype(jnp.int32)
    slot_order = row_orders(key_slot, DEVICES, G_DEV).astype(jnp.int32)
    block_of = local_order // CAP
    pre_owner = (block_of + shift[:, None]) % DEVICES
    owner_dev = label[pre_owner]
    slot_in = slot_order[pre_owner, local_order]
    return (owner_dev * G_DEV + slot_in).astype(jnp.int32)


def place_ends(result, key, least, largest):
    index_at = [jax.random.randint(jax.random.fold_in(key, axis), (), 0, length) for axis, length in enumerate(result.shape)]
    widest = result.shape.index(max(result.shape))
    beside = index_at[:widest] + [(index_at[widest] + 1) % result.shape[widest]] + index_at[widest + 1:]
    return result.at[tuple(index_at)].set(least).at[tuple(beside)].set(largest)


def steps_of(key, dims, cuts, smallest, high):
    factor_of = 1.0
    for dim, parts in cuts:
        steps = jax.random.uniform(jax.random.fold_in(jax.random.fold_in(key, 6), dim), (parts,), jnp.float32, smallest / len(cuts), high / len(cuts))
        factor_of = factor_of * jnp.repeat(jnp.exp(steps), dims[dim] // parts).reshape((-1,) + (1,) * (len(dims) - 1 - dim))
    return factor_of


def split_up(count, total, most, lean):
    loads = [(1 << 20) // math.isqrt(standing ** lean) + 1 for standing in range(2, count + 1)]
    spare, counts = total - most - (count - 1), [1] * (count - 1)
    while spare > 0:
        candidates = [i for i in range(count - 1) if counts[i] < most]
        mass, left = sum([loads[i] for i in candidates]), spare
        for i in candidates:
            more = min(most - counts[i], max(1, left * loads[i] // mass), spare)
            counts[i] = counts[i] + more
            spare = spare - more
    return np.array([most] + counts)


def ragged(own_key, number_of, total, most, slope):
    if number_of == 2:
        one = jax.random.randint(own_key, (), max(1, total - most), min(most, total - 1) + 1)
        return jnp.stack([one, total - one])
    tallies = jnp.asarray(split_up(number_of, total, most, slope), jnp.int32)
    couples = (number_of - 1) // 2
    giver, sink = tallies[1:1 + 2 * couples:2], tallies[2:2 + 2 * couples:2]
    margin = jnp.minimum(giver - 1, most - sink)
    passed = jax.random.randint(jax.random.fold_in(own_key, 1), (couples,), 0, 1 << 20) % (margin + 1)
    tallies = tallies.at[1:1 + 2 * couples:2].set(giver - passed).at[2:2 + 2 * couples:2].set(sink + passed)
    return tallies[jax.random.permutation(jax.random.fold_in(own_key, 2), number_of)]


def gaussian(rng, dims, deviation, reach, pieces=(), kind=jnp.bfloat16):
    factor_of = steps_of(rng, dims, pieces, -0.22, 0.18) if pieces else 1.0
    array = jax.random.normal(rng, dims, jnp.float32) * deviation * factor_of
    return jnp.minimum(jnp.maximum(array, -reach), reach).astype(kind)


def setup_inputs(seed: int = 0) -> dict:
    seeds = jax.random.split(jax.random.key(seed), 14)
    flux = gaussian(seeds[0], (DEVICES, P_DEV, NV), 1.0, 6.0, ((0, 512),), jnp.float32)
    patch_pft = place_ends(jax.random.randint(seeds[1], (DEVICES, P_DEV), 0, NPFT), jax.random.fold_in(seeds[1], 1), 0, NPFT - 1).astype(jnp.int32)
    patch_wt = jnp.clip(jnp.exp(math.log(2.0) - 2.3025851 * jax.random.uniform(seeds[2], (DEVICES, P_DEV), jnp.float32) ** steps_of(seeds[2], (DEVICES, P_DEV), ((0, 512),), -0.2, 0.2)), 0.2, 2.0)
    patch_col = jax.vmap(lambda own: jnp.searchsorted(jnp.cumsum(ragged(own, C_DEV, P_DEV, 4, 1)), jnp.arange(P_DEV), side="right"))(jax.random.split(seeds[3], DEVICES)).reshape((DEVICES, P_DEV)).astype(jnp.int32)
    col_wt = jnp.clip(jnp.exp(math.log(2.0) - 2.3025851 * jax.random.uniform(seeds[4], (DEVICES, C_DEV), jnp.float32) ** steps_of(seeds[4], (DEVICES, C_DEV), ((0, 512),), -0.2, 0.2)), 0.2, 2.0)
    col_lu = jax.vmap(lambda own: jnp.searchsorted(jnp.cumsum(ragged(own, L_DEV, C_DEV, 4, 1)), jnp.arange(C_DEV), side="right"))(jax.random.split(seeds[5], DEVICES)).reshape((DEVICES, C_DEV)).astype(jnp.int32)
    lu_wt = jnp.clip(jnp.exp(math.log(2.0) - 2.3025851 * jax.random.uniform(seeds[6], (DEVICES, L_DEV), jnp.float32) ** steps_of(seeds[6], (DEVICES, L_DEV), ((0, 512),), -0.2, 0.2)), 0.2, 2.0)
    lu_grid = jax.vmap(lambda own: jnp.searchsorted(jnp.cumsum(ragged(own, G_DEV, L_DEV, 4, 1)), jnp.arange(L_DEV), side="right"))(jax.random.split(seeds[7], DEVICES)).reshape((DEVICES, L_DEV)).astype(jnp.int32)
    cell_target = draw_cell_target(jax.random.fold_in(seeds[13], 71), 0)
    patch_count = place_ends(jax.random.randint(seeds[9], (DEVICES,), P_DEV // 16, P_DEV + 1), jax.random.fold_in(seeds[9], 1), P_DEV // 16, P_DEV).astype(jnp.int32)
    pft_scale = jnp.clip(jnp.exp(jax.random.uniform(seeds[10], (NPFT, NV), jnp.float32, math.log(0.3), math.log(3.0))), 0.3, 3.0)
    cpl_frac = jnp.clip(0.2 + 0.7 * jax.random.uniform(seeds[11], (GRID,), jnp.float32) ** steps_of(seeds[11], (GRID,), ((0, 512),), -0.2, 0.2), 0.2, 0.9)
    cpl_field = gaussian(seeds[12], (GRID, NV), 1.0, 6.0, ((0, 512),), jnp.float32)
    return {"flux": flux, "patch_pft": patch_pft, "patch_wt": patch_wt, "patch_col": patch_col, "col_wt": col_wt, "col_lu": col_lu, "lu_wt": lu_wt, "lu_grid": lu_grid, "cell_target": cell_target, "patch_count": patch_count, "pft_scale": pft_scale, "cpl_frac": cpl_frac, "cpl_field": cpl_field}


def reference(flux, patch_pft, patch_wt, patch_col, col_wt, col_lu, lu_wt, lu_grid, cell_target, patch_count, pft_scale, cpl_frac, cpl_field):
    position = jnp.arange(P_DEV, dtype=jnp.int32)

    def local_means(entries):
        values, pft_ids, pweight, columns, cweight, colland, lweight, lugrid, live_count = entries
        alive_mask = (position < live_count).astype(jnp.float32)
        scaled = values * pft_scale[pft_ids]
        land_of = colland[columns]
        home_of = lugrid[land_of]
        weight_eff = alive_mask * pweight * cweight[columns] * lweight[land_of]
        numer = jax.ops.segment_sum(scaled * weight_eff[:, None], home_of, G_DEV)
        denom = jax.ops.segment_sum(weight_eff, home_of, G_DEV)
        return numer / jnp.maximum(denom, 1.0)[:, None]

    cell_mean = lax.map(local_means, (flux, patch_pft, patch_wt, patch_col, col_wt, col_lu, lu_wt, lu_grid, patch_count))
    placed = jnp.zeros((GRID, NV), jnp.float32).at[cell_target.reshape(-1)].set(cell_mean.reshape(-1, NV))
    grid_merged = cpl_frac[:, None] * placed + (1.0 - cpl_frac)[:, None] * cpl_field

    def local_anomaly(entries):
        values, pft_ids, columns, colland, lugrid, targets, live_count = entries
        alive_mask = (position < live_count).astype(jnp.float32)
        scaled = values * pft_scale[pft_ids]
        home_of = lugrid[colland[columns]]
        cell_merged = grid_merged[targets]
        return alive_mask[:, None] * (scaled - cell_merged[home_of])

    anomaly = lax.map(local_anomaly, (flux, patch_pft, patch_col, col_lu, lu_grid, cell_target, patch_count))
    return grid_merged, anomaly
```

```python
import jax
import jax.numpy as jnp
from jax import lax
from jax.experimental import pallas as pl
from jax.experimental.pallas import tpu as pltpu
from jax.sharding import PartitionSpec as P

F32 = jnp.float32
BF16 = jnp.bfloat16
AXES = ("clump", "grp")


def pieces(x, count):
    parts = []
    for _ in range(count):
        part = x.astype(BF16)
        parts.append(part)
        x = x - part.astype(F32)
    return parts


def contract(a, b, da, db):
    return lax.dot_general(a, b, (((da,), (db,)), ((), ())), preferred_element_type=F32)


def onehot(mask):
    return jnp.where(mask, F32(1.0), F32(0.0)).astype(BF16)


def iota(shape, dim):
    return lax.broadcasted_iota(jnp.int32, shape, dim)


def pair_masks(target, cells, devices):
    owner = target // cells
    owner_rows = jnp.broadcast_to(owner, (cells, cells)).astype(F32)
    same = owner_rows.T == owner_rows
    earlier = iota((cells, cells), 0) < iota((cells, cells), 1)
    rank = jnp.max(jnp.where(same & earlier, F32(1.0), F32(0.0)), axis=0, keepdims=True)
    hit = iota((devices, cells), 0) == owner
    return onehot(hit & (rank < 0.5)), onehot(hit & (rank > 0.5))


def side_by_side(x):
    hi, lo = pieces(x, 2)
    both = jnp.concatenate([hi, lo], axis=1)
    zero = jnp.zeros_like(both)
    return jnp.concatenate(
        [jnp.concatenate([both, zero], axis=1), jnp.concatenate([zero, both], axis=1)], axis=0
    )


def from_rows(rows, first, second):
    width = rows.shape[1] // 2
    hi, lo = pieces(rows, 2)
    one = contract(hi, first, 0, 0) + contract(lo, first, 0, 0)
    two = contract(hi, second, 0, 0) + contract(lo, second, 0, 0)
    return one[:width] + two[width:]


def gather_kernel(
    count_ref,
    flux_ref,
    pft_ref,
    wt_ref,
    col_ref,
    col_wt_ref,
    col_lu_ref,
    lu_wt_ref,
    lu_grid_ref,
    target_ref,
    scale_ref,
    send_ref,
    scaled_ref,
    home_ref,
):
    width, patches = flux_ref.shape
    cells = target_ref.shape[1]
    devices = send_ref.shape[0] // 2
    columns = col_wt_ref.shape[1]
    units = lu_wt_ref.shape[1]
    types = scale_ref.shape[0]

    unit_table = jnp.concatenate(
        pieces(lu_wt_ref[...], 3)
        + [lu_grid_ref[...].astype(F32).astype(BF16), jnp.zeros((12, units), BF16)],
        axis=0,
    )
    unit_of = onehot(iota((units, columns), 0) == col_lu_ref[...])
    picked = contract(unit_table, unit_of, 1, 0)
    col_weight = col_wt_ref[...] * (picked[0:1] + picked[1:2] + picked[2:3])
    col_table = jnp.concatenate(
        pieces(col_weight, 3) + [picked[3:4].astype(BF16), jnp.zeros((12, columns), BF16)], axis=0
    )
    col_of = onehot(iota((columns, patches), 0) == col_ref[...])
    picked = contract(col_table, col_of, 1, 0)
    alive = iota((1, patches), 1) < count_ref[0]
    weight = jnp.where(
        alive, wt_ref[...] * (picked[0:1] + picked[1:2] + picked[2:3]), F32(0.0)
    )
    home = picked[3:4].astype(jnp.int32)
    home_ref[...] = home

    type_of = onehot(iota((types, patches), 0) == pft_ref[...])
    scale_parts = jnp.concatenate(pieces(scale_ref[...], 3), axis=0)
    factor = contract(scale_parts, jnp.concatenate([type_of] * 3, axis=0), 0, 0)
    scaled = flux_ref[...] * factor
    scaled_ref[...] = scaled

    cell_of = onehot(iota((cells, patches), 0) == home)
    terms = jnp.concatenate([scaled * weight, weight, jnp.zeros((15, patches), F32)], axis=0)
    sums = [contract(part, cell_of, 1, 1) for part in pieces(terms, 2)]
    total = sums[0] + sums[1]
    mean = total[:width] / jnp.maximum(total[width : width + 1], 1.0)

    first, second = pair_masks(target_ref[...], cells, devices)
    masks = jnp.concatenate([first, first, second, second], axis=1)
    send_ref[pl.ds(0, devices, 2), :] = contract(masks, side_by_side(mean), 1, 1)
    slot = (target_ref[...] % cells + 1).astype(F32).astype(BF16)
    pad = jnp.zeros((1, cells), BF16)
    slot_rows = jnp.concatenate(
        [
            jnp.concatenate([slot, pad, pad, pad], axis=1),
            jnp.concatenate([pad, pad, slot, pad], axis=1),
            jnp.zeros((2 * width - 2, 4 * cells), BF16),
        ],
        axis=0,
    )
    send_ref[pl.ds(1, devices, 2), :] = contract(masks, slot_rows, 1, 1)


def merge_kernel(got_ref, frac_ref, field_ref, merged_ref, reply_ref):
    width, cells = field_ref.shape
    devices = reply_ref.shape[0]
    rows = got_ref[pl.ds(0, devices, 2), :]
    slots = got_ref[pl.ds(1, devices, 2), :].astype(jnp.int32) - 1
    lane = iota((devices, cells), 1)
    first = onehot(lane == slots[:, 0:1])
    second = onehot(lane == slots[:, 1:2])
    frac = frac_ref[...]
    merged = frac * from_rows(rows, first, second) + (1.0 - frac) * field_ref[...]
    merged_ref[...] = merged
    masks = jnp.concatenate([first, first, second, second], axis=1)
    reply_ref[...] = contract(masks, side_by_side(merged), 1, 1)


def spread_kernel(count_ref, back_ref, target_ref, home_ref, scaled_ref, out_ref):
    width, patches = scaled_ref.shape
    cells = target_ref.shape[1]
    devices = back_ref.shape[0]
    first, second = pair_masks(target_ref[...], cells, devices)
    merged = from_rows(back_ref[...], first, second)
    cell_of = onehot(iota((cells, patches), 0) == home_ref[...])
    parts = contract(jnp.concatenate(pieces(merged, 2), axis=0), cell_of, 1, 0)
    picked = parts[:width] + parts[width:]
    alive = iota((1, patches), 1) < count_ref[0]
    out_ref[...] = jnp.where(alive, scaled_ref[...] - picked, F32(0.0))


VMEM = pl.BlockSpec(memory_space=pltpu.VMEM)
SMEM = pl.BlockSpec(memory_space=pltpu.SMEM)


def exchange(x):
    return lax.all_to_all(x, AXES, split_axis=0, concat_axis=0, tiled=True)


def per_device(
    flux,
    patch_pft,
    patch_wt,
    patch_col,
    col_wt,
    col_lu,
    lu_wt,
    lu_grid,
    cell_target,
    patch_count,
    pft_scale,
    cpl_frac,
    cpl_field,
):
    devices = lax.axis_size("clump") * lax.axis_size("grp")
    patches, width = flux.shape[1:]
    cells = cell_target.shape[1]
    shape = jax.ShapeDtypeStruct
    send, scaled, home = pl.pallas_call(
        gather_kernel,
        out_shape=(
            shape((2 * devices, 2 * width), F32),
            shape((width, patches), F32),
            shape((1, patches), jnp.int32),
        ),
        in_specs=[SMEM] + [VMEM] * 10,
        out_specs=(VMEM, VMEM, VMEM),
        name="gather_cells",
    )(
        patch_count,
        flux[0].T,
        patch_pft,
        patch_wt,
        patch_col,
        col_wt,
        col_lu,
        lu_wt,
        lu_grid,
        cell_target,
        pft_scale,
    )
    got = exchange(send.reshape(devices, 2, 2 * width)).reshape(2 * devices, 2 * width)
    merged, reply = pl.pallas_call(
        merge_kernel,
        out_shape=(shape((width, cells), F32), shape((devices, 2 * width), F32)),
        in_specs=[VMEM] * 3,
        out_specs=(VMEM, VMEM),
        name="merge_cells",
    )(got, cpl_frac.reshape(1, cells), cpl_field.T)
    back = exchange(reply.reshape(devices, 1, 2 * width)).reshape(devices, 2 * width)
    anomaly = pl.pallas_call(
        spread_kernel,
        out_shape=shape((width, patches), F32),
        in_specs=[SMEM] + [VMEM] * 4,
        out_specs=VMEM,
        name="spread_cells",
    )(patch_count, back, cell_target, home, scaled)
    return merged.T, anomaly.T[None]


def solution(mesh):
    rows = P(AXES, None)
    return jax.shard_map(
        per_device,
        mesh=mesh,
        in_specs=(
            P(AXES, None, None),
            rows,
            rows,
            rows,
            rows,
            rows,
            rows,
            rows,
            rows,
            P(AXES),
            P(),
            P(AXES),
            rows,
        ),
        out_specs=(rows, P(AXES, None, None)),
        check_vma=False,
    )
```

```python
import jax
import jax.numpy as jnp
from jax import lax
from jax.experimental import pallas as pl
from jax.experimental.pallas import tpu as pltpu
from jax.sharding import PartitionSpec as P

F32 = jnp.float32
BF16 = jnp.bfloat16
AXES = ("clump", "grp")
PLANES = 16


def pieces(x, count):
    parts = []
    for _ in range(count):
        part = x.astype(BF16)
        parts.append(part)
        x = x - part.astype(F32)
    return parts


def contract(a, b, da, db):
    return lax.dot_general(a, b, (((da,), (db,)), ((), ())), preferred_element_type=F32)


def onehot(mask):
    return jnp.where(mask, F32(1.0), F32(0.0)).astype(BF16)


def iota(shape, dim):
    return lax.broadcasted_iota(jnp.int32, shape, dim)


def earlier_mate(owner, cells):
    owner_rows = jnp.broadcast_to(owner, (cells, cells)).astype(F32)
    same = owner_rows.T == owner_rows
    earlier = iota((cells, cells), 0) < iota((cells, cells), 1)
    return jnp.max(jnp.where(same & earlier, F32(1.0), F32(0.0)), axis=0, keepdims=True)


def pair_masks(target, cells, devices):
    owner = target // cells
    rank = earlier_mate(owner, cells)
    hit = iota((devices, cells), 0) == owner
    return onehot(hit & (rank < 0.5)), onehot(hit & (rank > 0.5))


def side_by_side(x):
    hi, lo = pieces(x, 2)
    both = jnp.concatenate([hi, lo], axis=1)
    zero = jnp.zeros_like(both)
    return jnp.concatenate(
        [jnp.concatenate([both, zero], axis=1), jnp.concatenate([zero, both], axis=1)], axis=0
    )


def from_rows(rows, first, second):
    width = rows.shape[1] // 2
    hi, lo = pieces(rows, 2)
    one = contract(hi, first, 0, 0) + contract(lo, first, 0, 0)
    two = contract(hi, second, 0, 0) + contract(lo, second, 0, 0)
    return one[:width] + two[width:]


def gather_kernel(
    count_ref,
    flux_ref,
    pft_ref,
    wt_ref,
    col_ref,
    col_wt_ref,
    col_lu_ref,
    lu_wt_ref,
    lu_grid_ref,
    target_ref,
    scale_ref,
    send_ref,
    scaled_ref,
    cell_of_ref,
    first_ref,
    second_ref,
    *scratch,
):
    held, sems = scratch[:-1], scratch[-1]
    given = (
        col_lu_ref,
        lu_wt_ref,
        lu_grid_ref,
        col_wt_ref,
        col_ref,
        pft_ref,
        scale_ref,
        wt_ref,
        target_ref,
        flux_ref,
    )
    copies = [
        pltpu.make_async_copy(src, dst, sems.at[i]) for i, (src, dst) in enumerate(zip(given, held))
    ]
    for copy in copies:
        copy.start()
    (
        col_lu_ref,
        lu_wt_ref,
        lu_grid_ref,
        col_wt_ref,
        col_ref,
        pft_ref,
        scale_ref,
        wt_ref,
        target_ref,
        flux_ref,
    ) = held
    for copy in copies[:4]:
        copy.wait()
    width, patches = flux_ref.shape
    cells = target_ref.shape[1]
    devices = send_ref.shape[0] - PLANES
    columns = col_wt_ref.shape[1]
    units = lu_wt_ref.shape[1]
    types = scale_ref.shape[0]

    unit_table = jnp.concatenate(
        pieces(lu_wt_ref[...], 3)
        + [lu_grid_ref[...].astype(F32).astype(BF16), jnp.zeros((12, units), BF16)],
        axis=0,
    )
    unit_of = onehot(iota((units, columns), 0) == col_lu_ref[...])
    picked = contract(unit_table, unit_of, 1, 0)
    col_weight = col_wt_ref[...] * (picked[0:1] + picked[1:2] + picked[2:3])
    col_table = jnp.concatenate(
        pieces(col_weight, 3) + [picked[3:4].astype(BF16), jnp.zeros((12, columns), BF16)], axis=0
    )
    copies[4].wait()
    col_of = onehot(iota((columns, patches), 0) == col_ref[...])
    picked = contract(col_table, col_of, 1, 0)
    alive = iota((1, patches), 1) < count_ref[0]
    copies[7].wait()
    weight = jnp.where(
        alive, wt_ref[...] * (picked[0:1] + picked[1:2] + picked[2:3]), F32(0.0)
    )
    home = picked[3:4].astype(jnp.int32)

    copies[5].wait()
    copies[6].wait()
    type_of = onehot(iota((types, patches), 0) == pft_ref[...])
    scale_parts = jnp.concatenate(pieces(scale_ref[...], 3), axis=0)
    factor = contract(scale_parts, jnp.concatenate([type_of] * 3, axis=0), 0, 0)
    copies[9].wait()
    scaled = flux_ref[...] * factor
    scaled_ref[...] = scaled

    cell_of = onehot(iota((cells, patches), 0) == home)
    cell_of_ref[...] = cell_of
    terms = jnp.concatenate([scaled * weight, weight, jnp.zeros((15, patches), F32)], axis=0)
    sums = [contract(part, cell_of, 1, 1) for part in pieces(terms, 2)]
    total = sums[0] + sums[1]
    mean = total[:width] / jnp.maximum(total[width : width + 1], 1.0)

    copies[8].wait()
    first, second = pair_masks(target_ref[...], cells, devices)
    first_ref[...] = first
    second_ref[...] = second
    masks = jnp.concatenate([first, first, second, second], axis=1)
    rows = contract(masks, side_by_side(mean), 1, 1)
    plane = devices // PLANES
    target = target_ref[...]
    slot = (target % cells + 1).astype(F32)
    owner = target // cells
    rank = earlier_mate(owner, cells)
    lane = owner % plane + jnp.where(rank > 0.5, plane, 0)
    left = jnp.where(iota((PLANES, cells), 0) == owner // plane, slot, F32(0.0)).astype(BF16)
    right = onehot(iota((2 * width, cells), 0) == lane)
    slots = contract(left, right, 1, 1)
    for z in range(PLANES):
        send_ref[pl.ds(z * (plane + 1), plane), :] = rows[z * plane : (z + 1) * plane]
    send_ref[pl.ds(plane, PLANES, plane + 1), :] = slots


def turn_kernel(got_ref, send_ref):
    place = got_ref.shape[0] // PLANES - 1
    for z in range(PLANES):
        rows = got_ref[pl.ds(z * (place + 1), place), :]
        send_ref[pl.ds(z, place, PLANES + 1), :] = rows
    slots = got_ref[pl.ds(place, PLANES, place + 1), :]
    lanes = slots.shape[1]
    turned = jnp.concatenate([slots, jnp.zeros((lanes - PLANES, lanes), F32)], axis=0).T
    one, two = turned[:place], turned[place : 2 * place]
    send_ref[pl.ds(PLANES, place, PLANES + 1), :] = one + pltpu.roll(two, PLANES, 1)


def merge_kernel(got_ref, frac_ref, field_ref, merged_ref, reply_ref):
    width, cells = field_ref.shape
    devices = reply_ref.shape[0]
    place = devices // PLANES
    rows = jnp.concatenate(
        [got_ref[pl.ds(z, place, PLANES + 1), :] for z in range(PLANES)], axis=0
    )
    slots = got_ref[pl.ds(PLANES, place, PLANES + 1), :].astype(jnp.int32) - 1
    lane = iota((place, cells), 1)
    first, second = (
        jnp.concatenate(
            [onehot(lane == slots[:, k + z : k + z + 1]) for z in range(PLANES)], axis=0
        )
        for k in (0, PLANES)
    )
    frac = frac_ref[...]
    merged = frac * from_rows(rows, first, second) + (1.0 - frac) * field_ref[...]
    merged_ref[...] = merged
    masks = jnp.concatenate([first, first, second, second], axis=1)
    reply_ref[...] = contract(masks, side_by_side(merged), 1, 1)


def spread_kernel(count_ref, back_ref, first_ref, second_ref, cell_of_ref, scaled_ref, out_ref):
    width, patches = scaled_ref.shape
    merged = from_rows(back_ref[...], first_ref[...], second_ref[...])
    parts = contract(jnp.concatenate(pieces(merged, 2), axis=0), cell_of_ref[...], 1, 0)
    picked = parts[:width] + parts[width:]
    alive = iota((1, patches), 1) < count_ref[0]
    out_ref[...] = jnp.where(alive, scaled_ref[...] - picked, F32(0.0))


PARAMS = pltpu.CompilerParams(vmem_limit_bytes=12 << 20)
VMEM = pl.BlockSpec(memory_space=pltpu.VMEM)
HBM = pl.BlockSpec(memory_space=pltpu.HBM)
SMEM = pl.BlockSpec(memory_space=pltpu.SMEM)


def exchange(x, axis=AXES, groups=None):
    return lax.all_to_all(
        x, axis, split_axis=0, concat_axis=0, tiled=True, axis_index_groups=groups
    )


def per_device(
    flux,
    patch_pft,
    patch_wt,
    patch_col,
    col_wt,
    col_lu,
    lu_wt,
    lu_grid,
    cell_target,
    patch_count,
    pft_scale,
    cpl_frac,
    cpl_field,
):
    devices = lax.axis_size("clump") * lax.axis_size("grp")
    patches, width = flux.shape[1:]
    cells = cell_target.shape[1]
    shape = jax.ShapeDtypeStruct
    lanes = 2 * width
    place = devices // PLANES
    columns = lax.axis_size("clump") // PLANES
    along = [[z * columns + i for z in range(PLANES)] for i in range(columns)]
    across = [[z * place + i for i in range(place)] for z in range(PLANES)]
    send, scaled, cell_of, first, second = pl.pallas_call(
        gather_kernel,
        out_shape=(
            shape((devices + PLANES, lanes), F32),
            shape((width, patches), F32),
            shape((cells, patches), BF16),
            shape((devices, cells), BF16),
            shape((devices, cells), BF16),
        ),
        in_specs=[SMEM] + [HBM] * 10,
        out_specs=(VMEM,) * 5,
        scratch_shapes=[
            pltpu.VMEM(col_lu.shape, jnp.int32),
            pltpu.VMEM(lu_wt.shape, F32),
            pltpu.VMEM(lu_grid.shape, jnp.int32),
            pltpu.VMEM(col_wt.shape, F32),
            pltpu.VMEM(patch_col.shape, jnp.int32),
            pltpu.VMEM(patch_pft.shape, jnp.int32),
            pltpu.VMEM(pft_scale.shape, F32),
            pltpu.VMEM(patch_wt.shape, F32),
            pltpu.VMEM(cell_target.shape, jnp.int32),
            pltpu.VMEM((width, patches), F32),
            pltpu.SemaphoreType.DMA((10,)),
        ],
        compiler_params=PARAMS,
        name="gather_cells",
    )(
        patch_count,
        *(
            pltpu.with_memory_space_constraint(x, pltpu.HBM)
            for x in (
                flux[0].T,
                patch_pft,
                patch_wt,
                patch_col,
                col_wt,
                col_lu,
                lu_wt,
                lu_grid,
                cell_target,
                pft_scale,
            )
        ),
    )
    got = exchange(send.reshape(PLANES, 1, (place + 1) * lanes), "clump", along)
    send = pl.pallas_call(
        turn_kernel,
        out_shape=shape((place * (PLANES + 1), lanes), F32),
        in_specs=[VMEM],
        out_specs=VMEM,
        compiler_params=PARAMS,
        name="turn_rows",
    )(got.reshape(PLANES * (place + 1), lanes))
    got = exchange(send.reshape(place, 1, (PLANES + 1) * lanes), AXES, across)
    got = got.reshape(place * (PLANES + 1), lanes)
    merged, reply = pl.pallas_call(
        merge_kernel,
        out_shape=(shape((width, cells), F32), shape((devices, 2 * width), F32)),
        in_specs=[VMEM] * 3,
        out_specs=(VMEM, VMEM),
        compiler_params=PARAMS,
        name="merge_cells",
    )(got, cpl_frac.reshape(1, cells), cpl_field.T)
    back = exchange(reply.reshape(devices, 1, 2 * width)).reshape(devices, 2 * width)
    anomaly = pl.pallas_call(
        spread_kernel,
        out_shape=shape((width, patches), F32),
        in_specs=[SMEM] + [VMEM] * 5,
        out_specs=VMEM,
        compiler_params=PARAMS,
        name="spread_cells",
    )(patch_count, back, first, second, cell_of, scaled)
    return merged.T, anomaly.T[None]


def solution(mesh):
    rows = P(AXES, None)
    return jax.shard_map(
        per_device,
        mesh=mesh,
        in_specs=(
            P(AXES, None, None),
            rows,
            rows,
            rows,
            rows,
            rows,
            rows,
            rows,
            rows,
            P(AXES),
            P(),
            P(AXES),
            rows,
        ),
        out_specs=(rows, P(AXES, None, None)),
        check_vma=False,
    )
```

```python
import jax
import jax.numpy as jnp
from jax import lax
from jax.experimental import pallas as pl
from jax.experimental.pallas import tpu as pltpu
from jax.sharding import PartitionSpec as P


F32 = jnp.float32
BF16 = jnp.bfloat16
AXES = ("clump", "grp")
PLANES = 16


def pieces(x, count):
    parts = []
    for _ in range(count):
        part = x.astype(BF16)
        parts.append(part)
        x = x - part.astype(F32)
    return parts


def contract(a, b, da, db):
    return lax.dot_general(a, b, (((da,), (db,)), ((), ())), preferred_element_type=F32)


def onehot(mask):
    return jnp.where(mask, F32(1.0), F32(0.0)).astype(BF16)


def iota(shape, dim):
    return lax.broadcasted_iota(jnp.int32, shape, dim)


def earlier_mate(owner, cells):
    owner_rows = jnp.broadcast_to(owner, (cells, cells)).astype(F32)
    same = owner_rows.T == owner_rows
    earlier = iota((cells, cells), 0) < iota((cells, cells), 1)
    return jnp.max(jnp.where(same & earlier, F32(1.0), F32(0.0)), axis=0, keepdims=True)


def pair_masks(target, cells, devices):
    owner = target // cells
    rank = earlier_mate(owner, cells)
    place = devices // PLANES
    hit = iota((devices, cells), 0) == owner % place * PLANES + owner // place
    return onehot(hit & (rank < 0.5)), onehot(hit & (rank > 0.5))


def side_by_side(x):
    hi, lo = pieces(x, 2)
    both = jnp.concatenate([hi, lo], axis=1)
    zero = jnp.zeros_like(both)
    return jnp.concatenate(
        [jnp.concatenate([both, zero], axis=1), jnp.concatenate([zero, both], axis=1)], axis=0
    )


def from_rows(rows, first, second):
    width = rows.shape[1] // 2
    hi, lo = pieces(rows, 2)
    one = contract(hi, first, 0, 0) + contract(lo, first, 0, 0)
    two = contract(hi, second, 0, 0) + contract(lo, second, 0, 0)
    return one[:width] + two[width:]


def gather_kernel(
    count_ref,
    flux_ref,
    pft_ref,
    wt_ref,
    col_ref,
    col_wt_ref,
    col_lu_ref,
    lu_wt_ref,
    lu_grid_ref,
    target_ref,
    scale_ref,
    field_ref,
    frac_ref,
    send_ref,
    table_ref,
    scaled_ref,
    cell_of_ref,
    first_ref,
    second_ref,
    *scratch,
):
    held, sems = scratch[:-1], scratch[-1]
    given = (
        col_lu_ref,
        lu_wt_ref,
        lu_grid_ref,
        col_wt_ref,
        col_ref,
        pft_ref,
        scale_ref,
        wt_ref,
        target_ref,
        flux_ref,
    )
    copies = [
        pltpu.make_async_copy(src, dst, sems.at[i]) for i, (src, dst) in enumerate(zip(given, held))
    ]
    tables = [
        pltpu.make_async_copy(field_ref, table_ref.at[pl.ds(0, field_ref.shape[0])], sems.at[10]),
        pltpu.make_async_copy(frac_ref, table_ref.at[pl.ds(field_ref.shape[0], 1)], sems.at[11]),
    ]
    for copy in copies + tables:
        copy.start()
    (
        col_lu_ref,
        lu_wt_ref,
        lu_grid_ref,
        col_wt_ref,
        col_ref,
        pft_ref,
        scale_ref,
        wt_ref,
        target_ref,
        flux_ref,
    ) = held
    for copy in copies[:4]:
        copy.wait()
    width, patches = flux_ref.shape
    cells = target_ref.shape[1]
    devices = send_ref.shape[0] // (PLANES + 1) * PLANES
    columns = col_wt_ref.shape[1]
    units = lu_wt_ref.shape[1]
    types = scale_ref.shape[0]

    unit_table = jnp.concatenate(
        pieces(lu_wt_ref[...], 3)
        + [lu_grid_ref[...].astype(F32).astype(BF16), jnp.zeros((12, units), BF16)],
        axis=0,
    )
    unit_of = onehot(iota((units, columns), 0) == col_lu_ref[...])
    picked = contract(unit_table, unit_of, 1, 0)
    col_weight = col_wt_ref[...] * (picked[0:1] + picked[1:2] + picked[2:3])
    col_table = jnp.concatenate(
        pieces(col_weight, 3) + [picked[3:4].astype(BF16), jnp.zeros((12, columns), BF16)], axis=0
    )
    copies[4].wait()
    col_of = onehot(iota((columns, patches), 0) == col_ref[...])
    picked = contract(col_table, col_of, 1, 0)
    alive = iota((1, patches), 1) < count_ref[0]
    copies[7].wait()
    weight = jnp.where(
        alive, wt_ref[...] * (picked[0:1] + picked[1:2] + picked[2:3]), F32(0.0)
    )
    home = picked[3:4].astype(jnp.int32)

    copies[5].wait()
    copies[6].wait()
    type_of = onehot(iota((types, patches), 0) == pft_ref[...])
    scale_parts = jnp.concatenate(pieces(scale_ref[...], 3), axis=0)
    factor = contract(scale_parts, jnp.concatenate([type_of] * 3, axis=0), 0, 0)
    copies[9].wait()
    scaled = flux_ref[...] * factor
    scaled_ref[...] = scaled

    cell_of = onehot(iota((cells, patches), 0) == home)
    cell_of_ref[...] = cell_of
    terms = jnp.concatenate([scaled * weight, weight, jnp.zeros((15, patches), F32)], axis=0)
    sums = [contract(part, cell_of, 1, 1) for part in pieces(terms, 2)]
    total = sums[0] + sums[1]
    mean = total[:width] / jnp.maximum(total[width : width + 1], 1.0)

    copies[8].wait()
    first, second = pair_masks(target_ref[...], cells, devices)
    first_ref[...] = first
    second_ref[...] = second
    masks = jnp.concatenate([first, first, second, second], axis=1)
    rows = contract(masks, side_by_side(mean), 1, 1)
    place = devices // PLANES
    target = target_ref[...]
    slot = (target % cells + 1).astype(F32)
    owner = target // cells
    rank = earlier_mate(owner, cells)
    lane = owner // place + jnp.where(rank > 0.5, PLANES, 0)
    left = jnp.where(iota((place, cells), 0) == owner % place, slot, F32(0.0)).astype(BF16)
    right = onehot(iota((2 * width, cells), 0) == lane)
    slots = contract(left, right, 1, 1)
    for i in range(place):
        send_ref[pl.ds(i * (PLANES + 1), PLANES), :] = rows[i * PLANES : (i + 1) * PLANES]
    send_ref[pl.ds(PLANES, place, PLANES + 1), :] = slots
    for copy in tables:
        copy.wait()


def turn_kernel(got_ref, send_ref):
    place = got_ref.shape[0] // (PLANES + 1)
    for z in range(PLANES):
        send_ref[pl.ds(z * (place + 1), place), :] = got_ref[pl.ds(z, place, PLANES + 1), :]
    slots = got_ref[pl.ds(PLANES, place, PLANES + 1), :]
    lanes = slots.shape[1]
    turned = jnp.concatenate([slots, jnp.zeros((lanes - place, lanes), F32)], axis=0).T
    one, two = turned[:PLANES], turned[PLANES : 2 * PLANES]
    send_ref[pl.ds(place, PLANES, place + 1), :] = one + pltpu.roll(two, place, 1)


def reply_kernel(got_ref, table_ref, reply_ref):
    place = got_ref.shape[0] // (PLANES + 1)
    width = table_ref.shape[1] - 1
    cells = table_ref.shape[2]
    slots = got_ref[pl.ds(PLANES, place, PLANES + 1), :].astype(jnp.int32) - 1
    lane = iota((place, cells), 1)
    for z in range(PLANES):
        first = onehot(lane == slots[:, z : z + 1])
        second = onehot(lane == slots[:, PLANES + z : PLANES + z + 1])
        masks = jnp.concatenate([first, first, second, second], axis=1)
        field = table_ref[z, :width, :]
        frac = jnp.broadcast_to(table_ref[z, width:, :], (width, cells))
        fields = contract(masks, side_by_side(field), 1, 1)
        fracs = contract(masks, side_by_side(frac), 1, 1)
        means = got_ref[pl.ds(z, place, PLANES + 1), :]
        reply_ref[pl.ds(z, place, PLANES), :] = fracs * means + (1.0 - fracs) * fields


def merge_kernel(got_ref, table_ref, merged_ref):
    width, cells = merged_ref.shape
    place = got_ref.shape[0] // PLANES - 1
    rows = jnp.concatenate(
        [got_ref[pl.ds(z * (place + 1), place), :] for z in range(PLANES)], axis=0
    )
    slots = got_ref[pl.ds(place, PLANES, place + 1), :]
    lanes = slots.shape[1]
    turned = jnp.concatenate([slots, jnp.zeros((lanes - PLANES, lanes), F32)], axis=0).T
    turned = turned.astype(jnp.int32) - 1
    lane = iota((place, cells), 1)
    first, second = (
        jnp.concatenate(
            [onehot(lane == turned[k : k + place, z : z + 1]) for z in range(PLANES)], axis=0
        )
        for k in (0, place)
    )
    field, frac = table_ref[:width, :], table_ref[width:, :]
    merged_ref[...] = frac * from_rows(rows, first, second) + (1.0 - frac) * field


def spread_kernel(count_ref, back_ref, first_ref, second_ref, cell_of_ref, scaled_ref, out_ref):
    width, patches = scaled_ref.shape
    merged = from_rows(back_ref[...], first_ref[...], second_ref[...])
    parts = contract(jnp.concatenate(pieces(merged, 2), axis=0), cell_of_ref[...], 1, 0)
    picked = parts[:width] + parts[width:]
    alive = iota((1, patches), 1) < count_ref[0]
    out_ref[...] = jnp.where(alive, scaled_ref[...] - picked, F32(0.0))


PARAMS = pltpu.CompilerParams(vmem_limit_bytes=12 << 20)
VMEM = pl.BlockSpec(memory_space=pltpu.VMEM)
HBM = pl.BlockSpec(memory_space=pltpu.HBM)
SMEM = pl.BlockSpec(memory_space=pltpu.SMEM)


def exchange(x, axis, groups):
    return lax.all_to_all(
        x, axis, split_axis=0, concat_axis=0, tiled=True, axis_index_groups=groups
    )


def per_device(
    flux,
    patch_pft,
    patch_wt,
    patch_col,
    col_wt,
    col_lu,
    lu_wt,
    lu_grid,
    cell_target,
    patch_count,
    pft_scale,
    cpl_frac,
    cpl_field,
):
    devices = lax.axis_size("clump") * lax.axis_size("grp")
    patches, width = flux.shape[1:]
    cells = cell_target.shape[1]
    shape = jax.ShapeDtypeStruct
    lanes = 2 * width
    place = devices // PLANES
    columns = lax.axis_size("clump") // PLANES
    along = [[z * columns + i for z in range(PLANES)] for i in range(columns)]
    across = [[z * place + i for i in range(place)] for z in range(PLANES)]
    send, table, scaled, cell_of, first, second = pl.pallas_call(
        gather_kernel,
        out_shape=(
            shape((place * (PLANES + 1), lanes), F32),
            shape((width + 1, cells), F32),
            shape((width, patches), F32),
            shape((cells, patches), BF16),
            shape((devices, cells), BF16),
            shape((devices, cells), BF16),
        ),
        in_specs=[SMEM] + [HBM] * 12,
        out_specs=(VMEM,) * 6,
        scratch_shapes=[
            pltpu.VMEM(col_lu.shape, jnp.int32),
            pltpu.VMEM(lu_wt.shape, F32),
            pltpu.VMEM(lu_grid.shape, jnp.int32),
            pltpu.VMEM(col_wt.shape, F32),
            pltpu.VMEM(patch_col.shape, jnp.int32),
            pltpu.VMEM(patch_pft.shape, jnp.int32),
            pltpu.VMEM(pft_scale.shape, F32),
            pltpu.VMEM(patch_wt.shape, F32),
            pltpu.VMEM(cell_target.shape, jnp.int32),
            pltpu.VMEM((width, patches), F32),
            pltpu.SemaphoreType.DMA((12,)),
        ],
        compiler_params=PARAMS,
        name="gather_cells",
    )(
        patch_count,
        *(
            pltpu.with_memory_space_constraint(x, pltpu.HBM)
            for x in (
                flux[0].T,
                patch_pft,
                patch_wt,
                patch_col,
                col_wt,
                col_lu,
                lu_wt,
                lu_grid,
                cell_target,
                pft_scale,
                cpl_field.T,
                cpl_frac.reshape(1, cells),
            )
        ),
    )
    got = exchange(send.reshape(place, 1, (PLANES + 1) * lanes), AXES, across)
    got = got.reshape(place * (PLANES + 1), lanes)
    onward = pl.pallas_call(
        turn_kernel,
        out_shape=shape((PLANES * (place + 1), lanes), F32),
        in_specs=[VMEM],
        out_specs=VMEM,
        compiler_params=PARAMS,
        name="turn_rows",
    )(got)
    owned = exchange(onward.reshape(PLANES, 1, (place + 1) * lanes), "clump", along)
    owned = owned.reshape(PLANES * (place + 1), lanes)
    tables = lax.all_gather(table, "clump", axis=0, tiled=False, axis_index_groups=along)
    reply = pl.pallas_call(
        reply_kernel,
        out_shape=shape((devices, lanes), F32),
        in_specs=[VMEM] * 2,
        out_specs=VMEM,
        compiler_params=PARAMS,
        name="reply_rows",
    )(got, tables)
    back = exchange(reply.reshape(place, 1, PLANES * lanes), AXES, across)
    back = back.reshape(devices, lanes)
    merged = pl.pallas_call(
        merge_kernel,
        out_shape=shape((width, cells), F32),
        in_specs=[VMEM] * 2,
        out_specs=VMEM,
        compiler_params=PARAMS,
        name="merge_cells",
    )(owned, table)
    anomaly = pl.pallas_call(
        spread_kernel,
        out_shape=shape((width, patches), F32),
        in_specs=[SMEM] + [VMEM] * 5,
        out_specs=VMEM,
        compiler_params=PARAMS,
        name="spread_cells",
    )(patch_count, back, first, second, cell_of, scaled)
    return merged.T, anomaly.T[None]


def solution(mesh):
    rows = P(AXES, None)

    return jax.shard_map(
        per_device,
        mesh=mesh,
        in_specs=(
            P(AXES, None, None),
            rows,
            rows,
            rows,
            rows,
            rows,
            rows,
            rows,
            rows,
            P(AXES),
            P(),
            P(AXES),
            rows,
        ),
        out_specs=(rows, P(AXES, None, None)),
        check_vma=False,
    )
```

```python
import jax
import jax.numpy as jnp
from jax import lax
from jax.experimental import pallas as pl
from jax.experimental.pallas import tpu as pltpu
from jax.sharding import PartitionSpec as P

F32 = jnp.float32
BF16 = jnp.bfloat16
AXES = ("clump", "grp")
PLANES = 16


def pieces(x, count):
    parts = []
    for _ in range(count):
        part = x.astype(BF16)
        parts.append(part)
        x = x - part.astype(F32)
    return parts


def contract(a, b, da, db):
    return lax.dot_general(a, b, (((da,), (db,)), ((), ())), preferred_element_type=F32)


def onehot(mask):
    return jnp.where(mask, F32(1.0), F32(0.0)).astype(BF16)


def iota(shape, dim):
    return lax.broadcasted_iota(jnp.int32, shape, dim)


def earlier_mate(owner, cells):
    owner_rows = jnp.broadcast_to(owner, (cells, cells)).astype(F32)
    same = owner_rows.T == owner_rows
    earlier = iota((cells, cells), 0) < iota((cells, cells), 1)
    return jnp.max(jnp.where(same & earlier, F32(1.0), F32(0.0)), axis=0, keepdims=True)


def pair_masks(target, cells, devices):
    owner = target // cells
    rank = earlier_mate(owner, cells)
    hit = iota((devices, cells), 0) == owner
    return onehot(hit & (rank < 0.5)), onehot(hit & (rank > 0.5))


def side_by_side(x):
    hi, lo = pieces(x, 2)
    both = jnp.concatenate([hi, lo], axis=1)
    zero = jnp.zeros_like(both)
    return jnp.concatenate(
        [jnp.concatenate([both, zero], axis=1), jnp.concatenate([zero, both], axis=1)], axis=0
    )


def from_rows(rows, first, second):
    width = rows.shape[1] // 2
    hi, lo = pieces(rows, 2)
    one = contract(hi, first, 0, 0) + contract(lo, first, 0, 0)
    two = contract(hi, second, 0, 0) + contract(lo, second, 0, 0)
    return one[:width] + two[width:]


def gather_kernel(
    count_ref,
    flux_ref,
    pft_ref,
    wt_ref,
    col_ref,
    col_wt_ref,
    col_lu_ref,
    lu_wt_ref,
    lu_grid_ref,
    target_ref,
    scale_ref,
    field_ref,
    frac_ref,
    send_ref,
    table_ref,
    scaled_ref,
    cell_of_ref,
    first_ref,
    second_ref,
    *scratch,
):
    held, sems = scratch[:-1], scratch[-1]
    given = (
        col_lu_ref,
        lu_wt_ref,
        lu_grid_ref,
        col_wt_ref,
        col_ref,
        pft_ref,
        scale_ref,
        wt_ref,
        target_ref,
        flux_ref,
    )
    copies = [
        pltpu.make_async_copy(src, dst, sems.at[i]) for i, (src, dst) in enumerate(zip(given, held))
    ]
    tables = [
        pltpu.make_async_copy(field_ref, table_ref.at[pl.ds(0, field_ref.shape[0])], sems.at[10]),
        pltpu.make_async_copy(frac_ref, table_ref.at[pl.ds(field_ref.shape[0], 1)], sems.at[11]),
    ]
    for copy in copies + tables:
        copy.start()
    (
        col_lu_ref,
        lu_wt_ref,
        lu_grid_ref,
        col_wt_ref,
        col_ref,
        pft_ref,
        scale_ref,
        wt_ref,
        target_ref,
        flux_ref,
    ) = held
    for copy in copies[:4]:
        copy.wait()
    width, patches = flux_ref.shape
    cells = target_ref.shape[1]
    devices = send_ref.shape[0] - PLANES
    columns = col_wt_ref.shape[1]
    units = lu_wt_ref.shape[1]
    types = scale_ref.shape[0]

    unit_table = jnp.concatenate(
        pieces(lu_wt_ref[...], 3)
        + [lu_grid_ref[...].astype(F32).astype(BF16), jnp.zeros((12, units), BF16)],
        axis=0,
    )
    unit_of = onehot(iota((units, columns), 0) == col_lu_ref[...])
    picked = contract(unit_table, unit_of, 1, 0)
    col_weight = col_wt_ref[...] * (picked[0:1] + picked[1:2] + picked[2:3])
    col_table = jnp.concatenate(
        pieces(col_weight, 3) + [picked[3:4].astype(BF16), jnp.zeros((12, columns), BF16)], axis=0
    )
    copies[4].wait()
    col_of = onehot(iota((columns, patches), 0) == col_ref[...])
    picked = contract(col_table, col_of, 1, 0)
    alive = iota((1, patches), 1) < count_ref[0]
    copies[7].wait()
    weight = jnp.where(
        alive, wt_ref[...] * (picked[0:1] + picked[1:2] + picked[2:3]), F32(0.0)
    )
    home = picked[3:4].astype(jnp.int32)

    copies[5].wait()
    copies[6].wait()
    type_of = onehot(iota((types, patches), 0) == pft_ref[...])
    scale_parts = jnp.concatenate(pieces(scale_ref[...], 3), axis=0)
    factor = contract(scale_parts, jnp.concatenate([type_of] * 3, axis=0), 0, 0)
    copies[9].wait()
    scaled = flux_ref[...] * factor
    scaled_ref[...] = scaled

    cell_of = onehot(iota((cells, patches), 0) == home)
    cell_of_ref[...] = cell_of
    terms = jnp.concatenate([scaled * weight, weight, jnp.zeros((15, patches), F32)], axis=0)
    sums = [contract(part, cell_of, 1, 1) for part in pieces(terms, 2)]
    total = sums[0] + sums[1]
    mean = total[:width] / jnp.maximum(total[width : width + 1], 1.0)

    copies[8].wait()
    first, second = pair_masks(target_ref[...], cells, devices)
    first_ref[...] = first
    second_ref[...] = second
    masks = jnp.concatenate([first, first, second, second], axis=1)
    rows = contract(masks, side_by_side(mean), 1, 1)
    plane = devices // PLANES
    target = target_ref[...]
    slot = (target % cells + 1).astype(F32)
    owner = target // cells
    rank = earlier_mate(owner, cells)
    lane = owner % plane + jnp.where(rank > 0.5, plane, 0)
    left = jnp.where(iota((PLANES, cells), 0) == owner // plane, slot, F32(0.0)).astype(BF16)
    right = onehot(iota((2 * width, cells), 0) == lane)
    slots = contract(left, right, 1, 1)
    for z in range(PLANES):
        send_ref[pl.ds(z * (plane + 1), plane), :] = rows[z * plane : (z + 1) * plane]
    send_ref[pl.ds(plane, PLANES, plane + 1), :] = slots
    for copy in tables:
        copy.wait()


def turn_kernel(got_ref, send_ref):
    place = got_ref.shape[0] // PLANES - 1
    for z in range(PLANES):
        rows = got_ref[pl.ds(z * (place + 1), place), :]
        send_ref[pl.ds(z, place, PLANES + 1), :] = rows
    slots = got_ref[pl.ds(place, PLANES, place + 1), :]
    lanes = slots.shape[1]
    turned = jnp.concatenate([slots, jnp.zeros((lanes - PLANES, lanes), F32)], axis=0).T
    one, two = turned[:place], turned[place : 2 * place]
    send_ref[pl.ds(PLANES, place, PLANES + 1), :] = one + pltpu.roll(two, PLANES, 1)


def turn_back_kernel(got_ref, send_ref):
    place = got_ref.shape[0] // PLANES
    for z in range(PLANES):
        send_ref[pl.ds(z * place, place), :] = got_ref[pl.ds(z, place, PLANES), :]


def merge_kernel(got_ref, table_ref, merged_ref, reply_ref):
    width, cells = merged_ref.shape
    devices = reply_ref.shape[0]
    place = devices // PLANES
    rows = jnp.concatenate(
        [got_ref[pl.ds(z, place, PLANES + 1), :] for z in range(PLANES)], axis=0
    )
    slots = got_ref[pl.ds(PLANES, place, PLANES + 1), :].astype(jnp.int32) - 1
    lane = iota((place, cells), 1)
    first, second = (
        jnp.concatenate(
            [onehot(lane == slots[:, k + z : k + z + 1]) for z in range(PLANES)], axis=0
        )
        for k in (0, PLANES)
    )
    field, frac = table_ref[:width, :], table_ref[width:, :]
    merged = frac * from_rows(rows, first, second) + (1.0 - frac) * field
    merged_ref[...] = merged
    masks = jnp.concatenate([first, first, second, second], axis=1)
    rows = contract(masks, side_by_side(merged), 1, 1)
    for z in range(PLANES):
        reply_ref[pl.ds(z, place, PLANES), :] = rows[z * place : (z + 1) * place]


def spread_kernel(count_ref, back_ref, first_ref, second_ref, cell_of_ref, scaled_ref, out_ref):
    width, patches = scaled_ref.shape
    merged = from_rows(back_ref[...], first_ref[...], second_ref[...])
    parts = contract(jnp.concatenate(pieces(merged, 2), axis=0), cell_of_ref[...], 1, 0)
    picked = parts[:width] + parts[width:]
    alive = iota((1, patches), 1) < count_ref[0]
    out_ref[...] = jnp.where(alive, scaled_ref[...] - picked, F32(0.0))


PARAMS = pltpu.CompilerParams(vmem_limit_bytes=12 << 20)
VMEM = pl.BlockSpec(memory_space=pltpu.VMEM)
HBM = pl.BlockSpec(memory_space=pltpu.HBM)
SMEM = pl.BlockSpec(memory_space=pltpu.SMEM)


def exchange(x, axis, groups):
    return lax.all_to_all(
        x, axis, split_axis=0, concat_axis=0, tiled=True, axis_index_groups=groups
    )


def per_device(
    flux,
    patch_pft,
    patch_wt,
    patch_col,
    col_wt,
    col_lu,
    lu_wt,
    lu_grid,
    cell_target,
    patch_count,
    pft_scale,
    cpl_frac,
    cpl_field,
):
    devices = lax.axis_size("clump") * lax.axis_size("grp")
    patches, width = flux.shape[1:]
    cells = cell_target.shape[1]
    shape = jax.ShapeDtypeStruct
    lanes = 2 * width
    place = devices // PLANES
    columns = lax.axis_size("clump") // PLANES
    along = [[z * columns + i for z in range(PLANES)] for i in range(columns)]
    across = [[z * place + i for i in range(place)] for z in range(PLANES)]
    send, table, scaled, cell_of, first, second = pl.pallas_call(
        gather_kernel,
        out_shape=(
            shape((devices + PLANES, lanes), F32),
            shape((width + 1, cells), F32),
            shape((width, patches), F32),
            shape((cells, patches), BF16),
            shape((devices, cells), BF16),
            shape((devices, cells), BF16),
        ),
        in_specs=[SMEM] + [HBM] * 12,
        out_specs=(VMEM,) * 6,
        scratch_shapes=[
            pltpu.VMEM(col_lu.shape, jnp.int32),
            pltpu.VMEM(lu_wt.shape, F32),
            pltpu.VMEM(lu_grid.shape, jnp.int32),
            pltpu.VMEM(col_wt.shape, F32),
            pltpu.VMEM(patch_col.shape, jnp.int32),
            pltpu.VMEM(patch_pft.shape, jnp.int32),
            pltpu.VMEM(pft_scale.shape, F32),
            pltpu.VMEM(patch_wt.shape, F32),
            pltpu.VMEM(cell_target.shape, jnp.int32),
            pltpu.VMEM((width, patches), F32),
            pltpu.SemaphoreType.DMA((12,)),
        ],
        compiler_params=PARAMS,
        name="gather_cells",
    )(
        patch_count,
        *(
            pltpu.with_memory_space_constraint(x, pltpu.HBM)
            for x in (
                flux[0].T,
                patch_pft,
                patch_wt,
                patch_col,
                col_wt,
                col_lu,
                lu_wt,
                lu_grid,
                cell_target,
                pft_scale,
                cpl_field.T,
                cpl_frac.reshape(1, cells),
            )
        ),
    )
    got = exchange(send.reshape(PLANES, 1, (place + 1) * lanes), "clump", along)
    send = pl.pallas_call(
        turn_kernel,
        out_shape=shape((place * (PLANES + 1), lanes), F32),
        in_specs=[VMEM],
        out_specs=VMEM,
        compiler_params=PARAMS,
        name="turn_rows",
    )(got.reshape(PLANES * (place + 1), lanes))
    got = exchange(send.reshape(place, 1, (PLANES + 1) * lanes), AXES, across)
    got = got.reshape(place * (PLANES + 1), lanes)
    merged, reply = pl.pallas_call(
        merge_kernel,
        out_shape=(shape((width, cells), F32), shape((devices, 2 * width), F32)),
        in_specs=[VMEM] * 2,
        out_specs=(VMEM, VMEM),
        compiler_params=PARAMS,
        name="merge_cells",
    )(got, table)
    back = exchange(reply.reshape(place, 1, PLANES * lanes), AXES, across)
    back = pl.pallas_call(
        turn_back_kernel,
        out_shape=shape((devices, lanes), F32),
        in_specs=[VMEM],
        out_specs=VMEM,
        compiler_params=PARAMS,
        name="turn_back",
    )(back.reshape(devices, lanes))
    back = exchange(back.reshape(PLANES, 1, place * lanes), "clump", along)
    back = back.reshape(devices, lanes)
    anomaly = pl.pallas_call(
        spread_kernel,
        out_shape=shape((width, patches), F32),
        in_specs=[SMEM] + [VMEM] * 5,
        out_specs=VMEM,
        compiler_params=PARAMS,
        name="spread_cells",
    )(patch_count, back, first, second, cell_of, scaled)
    return merged.T, anomaly.T[None]


def solution(mesh):
    rows = P(AXES, None)
    return jax.shard_map(
        per_device,
        mesh=mesh,
        in_specs=(
            P(AXES, None, None),
            rows,
            rows,
            rows,
            rows,
            rows,
            rows,
            rows,
            rows,
            P(AXES),
            P(),
            P(AXES),
            rows,
        ),
        out_specs=(rows, P(AXES, None, None)),
        check_vma=False,
    )
```

```python
import jax
import jax.numpy as jnp
from jax import lax
from jax.experimental import pallas as pl
from jax.experimental.pallas import tpu as pltpu
from jax.sharding import PartitionSpec as P

F32 = jnp.float32
BF16 = jnp.bfloat16
AXES = ("clump", "grp")
PLANES = 16


def pieces(x, count):
    parts = []
    for _ in range(count):
        part = x.astype(BF16)
        parts.append(part)
        x = x - part.astype(F32)
    return parts


def contract(a, b, da, db):
    return lax.dot_general(a, b, (((da,), (db,)), ((), ())), preferred_element_type=F32)


def onehot(mask):
    return jnp.where(mask, F32(1.0), F32(0.0)).astype(BF16)


def iota(shape, dim):
    return lax.broadcasted_iota(jnp.int32, shape, dim)


def earlier_mate(owner, cells):
    owner_rows = jnp.broadcast_to(owner, (cells, cells)).astype(F32)
    same = owner_rows.T == owner_rows
    earlier = iota((cells, cells), 0) < iota((cells, cells), 1)
    return jnp.max(jnp.where(same & earlier, F32(1.0), F32(0.0)), axis=0, keepdims=True)


def ordered(owner):
    return owner // 8 * 8 + owner % 4 * 2 + owner // 4 % 2


def pair_masks(target, cells, devices):
    owner = ordered(target // cells)
    rank = earlier_mate(owner, cells)
    hit = iota((devices, cells), 0) == owner
    return onehot(hit & (rank < 0.5)), onehot(hit & (rank > 0.5))


def side_by_side(x):
    hi, lo = pieces(x, 2)
    both = jnp.concatenate([hi, lo], axis=1)
    zero = jnp.zeros_like(both)
    return jnp.concatenate(
        [jnp.concatenate([both, zero], axis=1), jnp.concatenate([zero, both], axis=1)], axis=0
    )


def from_rows(rows, first, second):
    width = rows.shape[1] // 2
    hi, lo = pieces(rows, 2)
    one = contract(hi, first, 0, 0) + contract(lo, first, 0, 0)
    two = contract(hi, second, 0, 0) + contract(lo, second, 0, 0)
    return one[:width] + two[width:]


def gather_kernel(
    count_ref,
    flux_ref,
    pft_ref,
    wt_ref,
    col_ref,
    col_wt_ref,
    col_lu_ref,
    lu_wt_ref,
    lu_grid_ref,
    target_ref,
    scale_ref,
    field_ref,
    frac_ref,
    send_ref,
    table_ref,
    scaled_ref,
    cell_of_ref,
    first_ref,
    second_ref,
    *scratch,
):
    held, sems = scratch[:-1], scratch[-1]
    given = (
        col_lu_ref,
        lu_wt_ref,
        lu_grid_ref,
        col_wt_ref,
        col_ref,
        pft_ref,
        scale_ref,
        wt_ref,
        target_ref,
        flux_ref,
    )
    copies = [
        pltpu.make_async_copy(src, dst, sems.at[i]) for i, (src, dst) in enumerate(zip(given, held))
    ]
    tables = [
        pltpu.make_async_copy(field_ref, table_ref.at[pl.ds(0, field_ref.shape[0])], sems.at[10]),
        pltpu.make_async_copy(frac_ref, table_ref.at[pl.ds(field_ref.shape[0], 1)], sems.at[11]),
    ]
    for copy in copies + tables:
        copy.start()
    (
        col_lu_ref,
        lu_wt_ref,
        lu_grid_ref,
        col_wt_ref,
        col_ref,
        pft_ref,
        scale_ref,
        wt_ref,
        target_ref,
        flux_ref,
    ) = held
    for copy in copies[:4]:
        copy.wait()
    width, patches = flux_ref.shape
    cells = target_ref.shape[1]
    devices = send_ref.shape[0] - PLANES
    columns = col_wt_ref.shape[1]
    units = lu_wt_ref.shape[1]
    types = scale_ref.shape[0]

    unit_table = jnp.concatenate(
        pieces(lu_wt_ref[...], 3)
        + [lu_grid_ref[...].astype(F32).astype(BF16), jnp.zeros((12, units), BF16)],
        axis=0,
    )
    unit_of = onehot(iota((units, columns), 0) == col_lu_ref[...])
    picked = contract(unit_table, unit_of, 1, 0)
    col_weight = col_wt_ref[...] * (picked[0:1] + picked[1:2] + picked[2:3])
    col_table = jnp.concatenate(
        pieces(col_weight, 3) + [picked[3:4].astype(BF16), jnp.zeros((12, columns), BF16)], axis=0
    )
    copies[4].wait()
    col_of = onehot(iota((columns, patches), 0) == col_ref[...])
    picked = contract(col_table, col_of, 1, 0)
    alive = iota((1, patches), 1) < count_ref[0]
    copies[7].wait()
    weight = jnp.where(
        alive, wt_ref[...] * (picked[0:1] + picked[1:2] + picked[2:3]), F32(0.0)
    )
    home = picked[3:4].astype(jnp.int32)

    copies[5].wait()
    copies[6].wait()
    type_of = onehot(iota((types, patches), 0) == pft_ref[...])
    scale_parts = jnp.concatenate(pieces(scale_ref[...], 3), axis=0)
    factor = contract(scale_parts, jnp.concatenate([type_of] * 3, axis=0), 0, 0)
    copies[9].wait()
    scaled = flux_ref[...] * factor
    scaled_ref[...] = scaled

    cell_of = onehot(iota((cells, patches), 0) == home)
    cell_of_ref[...] = cell_of
    terms = jnp.concatenate([scaled * weight, weight, jnp.zeros((15, patches), F32)], axis=0)
    sums = [contract(part, cell_of, 1, 1) for part in pieces(terms, 2)]
    total = sums[0] + sums[1]
    mean = total[:width] / jnp.maximum(total[width : width + 1], 1.0)

    copies[8].wait()
    first, second = pair_masks(target_ref[...], cells, devices)
    first_ref[...] = first
    second_ref[...] = second
    masks = jnp.concatenate([first, first, second, second], axis=1)
    rows = contract(masks, side_by_side(mean), 1, 1)
    plane = devices // PLANES
    target = target_ref[...]
    slot = (target % cells + 1).astype(F32)
    owner = ordered(target // cells)
    rank = earlier_mate(owner, cells)
    lane = owner % plane + jnp.where(rank > 0.5, plane, 0)
    left = jnp.where(iota((PLANES, cells), 0) == owner // plane, slot, F32(0.0)).astype(BF16)
    right = onehot(iota((2 * width, cells), 0) == lane)
    slots = contract(left, right, 1, 1)
    for z in range(PLANES):
        send_ref[pl.ds(z * (plane + 1), plane), :] = rows[z * plane : (z + 1) * plane]
    send_ref[pl.ds(plane, PLANES, plane + 1), :] = slots
    for copy in tables:
        copy.wait()


def turn_kernel(got_ref, send_ref):
    place = got_ref.shape[0] // PLANES - 1
    for z in range(PLANES):
        rows = got_ref[pl.ds(z * (place + 1), place), :]
        send_ref[pl.ds(z, place, PLANES + 1), :] = rows
    slots = got_ref[pl.ds(place, PLANES, place + 1), :]
    lanes = slots.shape[1]
    turned = jnp.concatenate([slots, jnp.zeros((lanes - PLANES, lanes), F32)], axis=0).T
    one, two = turned[:place], turned[place : 2 * place]
    send_ref[pl.ds(PLANES, place, PLANES + 1), :] = one + pltpu.roll(two, PLANES, 1)


def turn_back_kernel(got_ref, send_ref):
    chips = got_ref.shape[0] // 2
    for core in range(2):
        send_ref[pl.ds(core, chips, 2), :] = got_ref[pl.ds(core * chips, chips), :]


def merge_kernel(got_ref, table_ref, merged_ref, reply_ref):
    width, cells = merged_ref.shape
    devices = reply_ref.shape[0]
    half = devices // PLANES // 2
    step = PLANES + 1
    lane = iota((half, cells), 1)
    rows, first, second = [], [], []
    for core in range(2):
        slots = got_ref[pl.ds(core * step + PLANES, half, 2 * step), :].astype(jnp.int32) - 1
        for z in range(PLANES):
            rows.append(got_ref[pl.ds(core * step + z, half, 2 * step), :])
            first.append(onehot(lane == slots[:, z : z + 1]))
            second.append(onehot(lane == slots[:, PLANES + z : PLANES + z + 1]))
    rows, first, second = (jnp.concatenate(x, axis=0) for x in (rows, first, second))
    field, frac = table_ref[:width, :], table_ref[width:, :]
    merged = frac * from_rows(rows, first, second) + (1.0 - frac) * field
    merged_ref[...] = merged
    masks = jnp.concatenate([first, first, second, second], axis=1)
    reply_ref[...] = contract(masks, side_by_side(merged), 1, 1)


def spread_kernel(count_ref, back_ref, first_ref, second_ref, cell_of_ref, scaled_ref, out_ref):
    width, patches = scaled_ref.shape
    merged = from_rows(back_ref[...], first_ref[...], second_ref[...])
    parts = contract(jnp.concatenate(pieces(merged, 2), axis=0), cell_of_ref[...], 1, 0)
    picked = parts[:width] + parts[width:]
    alive = iota((1, patches), 1) < count_ref[0]
    out_ref[...] = jnp.where(alive, scaled_ref[...] - picked, F32(0.0))


PARAMS = pltpu.CompilerParams(vmem_limit_bytes=12 << 20)
VMEM = pl.BlockSpec(memory_space=pltpu.VMEM)
HBM = pl.BlockSpec(memory_space=pltpu.HBM)
SMEM = pl.BlockSpec(memory_space=pltpu.SMEM)


def exchange(x, axis, groups):
    return lax.all_to_all(
        x, axis, split_axis=0, concat_axis=0, tiled=True, axis_index_groups=groups
    )


def per_device(
    flux,
    patch_pft,
    patch_wt,
    patch_col,
    col_wt,
    col_lu,
    lu_wt,
    lu_grid,
    cell_target,
    patch_count,
    pft_scale,
    cpl_frac,
    cpl_field,
):
    devices = lax.axis_size("clump") * lax.axis_size("grp")
    patches, width = flux.shape[1:]
    cells = cell_target.shape[1]
    shape = jax.ShapeDtypeStruct
    lanes = 2 * width
    place = devices // PLANES
    columns = lax.axis_size("clump") // PLANES
    along = [[z * columns + i for z in range(PLANES)] for i in range(columns)]
    inner = [y * 8 + core * 4 + x for y in range(4) for x in range(4) for core in range(2)]
    across = [[z * place + i for i in inner] for z in range(PLANES)]
    chips = [
        [z * place + i for z in range(PLANES) for i in inner[core::2]] for core in range(2)
    ]
    cores = [[2 * i, 2 * i + 1] for i in range(lax.axis_size("clump") // 2)]
    send, table, scaled, cell_of, first, second = pl.pallas_call(
        gather_kernel,
        out_shape=(
            shape((devices + PLANES, lanes), F32),
            shape((width + 1, cells), F32),
            shape((width, patches), F32),
            shape((cells, patches), BF16),
            shape((devices, cells), BF16),
            shape((devices, cells), BF16),
        ),
        in_specs=[SMEM] + [HBM] * 12,
        out_specs=(VMEM,) * 6,
        scratch_shapes=[
            pltpu.VMEM(col_lu.shape, jnp.int32),
            pltpu.VMEM(lu_wt.shape, F32),
            pltpu.VMEM(lu_grid.shape, jnp.int32),
            pltpu.VMEM(col_wt.shape, F32),
            pltpu.VMEM(patch_col.shape, jnp.int32),
            pltpu.VMEM(patch_pft.shape, jnp.int32),
            pltpu.VMEM(pft_scale.shape, F32),
            pltpu.VMEM(patch_wt.shape, F32),
            pltpu.VMEM(cell_target.shape, jnp.int32),
            pltpu.VMEM((width, patches), F32),
            pltpu.SemaphoreType.DMA((12,)),
        ],
        compiler_params=PARAMS,
        name="gather_cells",
    )(
        patch_count,
        *(
            pltpu.with_memory_space_constraint(x, pltpu.HBM)
            for x in (
                flux[0].T,
                patch_pft,
                patch_wt,
                patch_col,
                col_wt,
                col_lu,
                lu_wt,
                lu_grid,
                cell_target,
                pft_scale,
                cpl_field.T,
                cpl_frac.reshape(1, cells),
            )
        ),
    )
    got = exchange(send.reshape(PLANES, 1, (place + 1) * lanes), "clump", along)
    send = pl.pallas_call(
        turn_kernel,
        out_shape=shape((place * (PLANES + 1), lanes), F32),
        in_specs=[VMEM],
        out_specs=VMEM,
        compiler_params=PARAMS,
        name="turn_rows",
    )(got.reshape(PLANES * (place + 1), lanes))
    got = exchange(send.reshape(place, 1, (PLANES + 1) * lanes), AXES, across)
    got = got.reshape(place * (PLANES + 1), lanes)
    merged, reply = pl.pallas_call(
        merge_kernel,
        out_shape=(shape((width, cells), F32), shape((devices, 2 * width), F32)),
        in_specs=[VMEM] * 2,
        out_specs=(VMEM, VMEM),
        compiler_params=PARAMS,
        name="merge_cells",
    )(got, table)
    back = exchange(reply.reshape(2, devices // 2, lanes), "clump", cores)
    back = pl.pallas_call(
        turn_back_kernel,
        out_shape=shape((devices, lanes), F32),
        in_specs=[VMEM],
        out_specs=VMEM,
        compiler_params=PARAMS,
        name="turn_back",
    )(back.reshape(devices, lanes))
    back = exchange(back.reshape(devices // 2, 2, lanes), AXES, chips)
    back = back.reshape(devices, lanes)
    anomaly = pl.pallas_call(
        spread_kernel,
        out_shape=shape((width, patches), F32),
        in_specs=[SMEM] + [VMEM] * 5,
        out_specs=VMEM,
        compiler_params=PARAMS,
        name="spread_cells",
    )(patch_count, back, first, second, cell_of, scaled)
    return merged.T, anomaly.T[None]


def solution(mesh):
    rows = P(AXES, None)
    return jax.shard_map(
        per_device,
        mesh=mesh,
        in_specs=(
            P(AXES, None, None),
            rows,
            rows,
            rows,
            rows,
            rows,
            rows,
            rows,
            rows,
            P(AXES),
            P(),
            P(AXES),
            rows,
        ),
        out_specs=(rows, P(AXES, None, None)),
        check_vma=False,
    )
```

```python
import functools

import jax
import jax.numpy as jnp
from jax import lax
from jax.experimental import pallas as pl
from jax.experimental.pallas import tpu as pltpu
from jax.sharding import PartitionSpec as P

F32 = jnp.float32
BF16 = jnp.bfloat16
AXES = ("clump", "grp")
PLANES = 16


def pieces(x, count):
    parts = []
    for _ in range(count):
        part = x.astype(BF16)
        parts.append(part)
        x = x - part.astype(F32)
    return parts


def contract(a, b, da, db):
    return lax.dot_general(a, b, (((da,), (db,)), ((), ())), preferred_element_type=F32)


def onehot(mask):
    return jnp.where(mask, F32(1.0), F32(0.0)).astype(BF16)


def iota(shape, dim):
    return lax.broadcasted_iota(jnp.int32, shape, dim)


def cell_rows(target, cells, devices):
    place = devices // PLANES
    owner = target // cells
    across = jnp.broadcast_to(owner, (cells, cells)).astype(F32)
    down = across.T
    base = jnp.broadcast_to(owner - owner % place, (cells, cells)).astype(F32)
    earlier = (down == across) & (iota((cells, cells), 0) < iota((cells, cells), 1))
    rank = jnp.max(jnp.where(earlier, F32(1.0), F32(0.0)), axis=0, keepdims=True)
    below = (down < across) & (down >= base)
    row = jnp.sum(jnp.where(below, F32(0.5), F32(0.0)), axis=0, keepdims=True)
    return owner // place, owner % place, rank > 0.5, row.astype(jnp.int32)


def side_by_side(x):
    hi, lo = pieces(x, 2)
    both = jnp.concatenate([hi, lo], axis=1)
    zero = jnp.zeros_like(both)
    return jnp.concatenate(
        [jnp.concatenate([both, zero], axis=1), jnp.concatenate([zero, both], axis=1)], axis=0
    )


def from_rows(rows, first, second):
    width = rows.shape[1] // 2
    hi, lo = pieces(rows, 2)
    one = contract(hi, first, 0, 0) + contract(lo, first, 0, 0)
    two = contract(hi, second, 0, 0) + contract(lo, second, 0, 0)
    return one[:width] + two[width:]


def gather_kernel(
    devices,
    count_ref,
    flux_ref,
    pft_ref,
    wt_ref,
    col_ref,
    col_wt_ref,
    col_lu_ref,
    lu_wt_ref,
    lu_grid_ref,
    target_ref,
    scale_ref,
    field_ref,
    frac_ref,
    send_ref,
    table_ref,
    scaled_ref,
    cell_of_ref,
    first_ref,
    second_ref,
    *scratch,
):
    held, sems = scratch[:-1], scratch[-1]
    given = (
        col_lu_ref,
        lu_wt_ref,
        lu_grid_ref,
        col_wt_ref,
        col_ref,
        pft_ref,
        scale_ref,
        wt_ref,
        target_ref,
        flux_ref,
    )
    copies = [
        pltpu.make_async_copy(src, dst, sems.at[i]) for i, (src, dst) in enumerate(zip(given, held))
    ]
    tables = [
        pltpu.make_async_copy(field_ref, table_ref.at[pl.ds(0, field_ref.shape[0])], sems.at[10]),
        pltpu.make_async_copy(frac_ref, table_ref.at[pl.ds(field_ref.shape[0], 1)], sems.at[11]),
    ]
    for copy in copies + tables:
        copy.start()
    (
        col_lu_ref,
        lu_wt_ref,
        lu_grid_ref,
        col_wt_ref,
        col_ref,
        pft_ref,
        scale_ref,
        wt_ref,
        target_ref,
        flux_ref,
    ) = held
    for copy in copies[:4]:
        copy.wait()
    width, patches = flux_ref.shape
    cells = target_ref.shape[1]
    room = send_ref.shape[0] // PLANES - 1
    lanes = send_ref.shape[1]
    columns = col_wt_ref.shape[1]
    units = lu_wt_ref.shape[1]
    types = scale_ref.shape[0]

    unit_table = jnp.concatenate(
        pieces(lu_wt_ref[...], 3)
        + [lu_grid_ref[...].astype(F32).astype(BF16), jnp.zeros((12, units), BF16)],
        axis=0,
    )
    unit_of = onehot(iota((units, columns), 0) == col_lu_ref[...])
    picked = contract(unit_table, unit_of, 1, 0)
    col_weight = col_wt_ref[...] * (picked[0:1] + picked[1:2] + picked[2:3])
    col_table = jnp.concatenate(
        pieces(col_weight, 3) + [picked[3:4].astype(BF16), jnp.zeros((12, columns), BF16)], axis=0
    )
    copies[4].wait()
    col_of = onehot(iota((columns, patches), 0) == col_ref[...])
    picked = contract(col_table, col_of, 1, 0)
    alive = iota((1, patches), 1) < count_ref[0]
    copies[7].wait()
    weight = jnp.where(
        alive, wt_ref[...] * (picked[0:1] + picked[1:2] + picked[2:3]), F32(0.0)
    )
    home = picked[3:4].astype(jnp.int32)

    copies[5].wait()
    copies[6].wait()
    type_of = onehot(iota((types, patches), 0) == pft_ref[...])
    scale_parts = jnp.concatenate(pieces(scale_ref[...], 3), axis=0)
    factor = contract(scale_parts, jnp.concatenate([type_of] * 3, axis=0), 0, 0)
    copies[9].wait()
    scaled = flux_ref[...] * factor
    scaled_ref[...] = scaled

    cell_of = onehot(iota((cells, patches), 0) == home)
    cell_of_ref[...] = cell_of
    terms = jnp.concatenate([scaled * weight, weight, jnp.zeros((15, patches), F32)], axis=0)
    sums = [contract(part, cell_of, 1, 1) for part in pieces(terms, 2)]
    total = sums[0] + sums[1]
    mean = total[:width] / jnp.maximum(total[width : width + 1], 1.0)

    copies[8].wait()
    target = target_ref[...]
    plane, place, second, row = cell_rows(target, cells, devices)
    hit = iota((PLANES * room, cells), 0) == plane * room + row
    one, two = onehot(hit & jnp.logical_not(second)), onehot(hit & second)
    first_ref[...] = one
    second_ref[...] = two
    rows = contract(jnp.concatenate([one, one, two, two], axis=1), side_by_side(mean), 1, 1)

    in_plane = iota((PLANES, cells), 0) == plane
    slot = (target % cells + 1).astype(F32)
    seat = jnp.where(second, F32(0.0), (place + 1).astype(F32))
    left = jnp.concatenate(
        [jnp.where(in_plane, seat, F32(0.0)), jnp.where(in_plane, slot, F32(0.0))], axis=1
    ).astype(BF16)
    lane = iota((lanes, cells), 0)
    right = jnp.concatenate(
        [onehot(lane == row), onehot(lane == row + jnp.where(second, 2 * room, room))], axis=1
    )
    notes = contract(left, right, 1, 1)
    full = jnp.where(jnp.max(row, axis=1, keepdims=True) < room, F32(0.0), F32(1.0))
    notes = jnp.where(iota((PLANES, lanes), 1) == lanes - 1, full, notes)
    for z in range(PLANES):
        send_ref[pl.ds(z * (room + 1), room), :] = rows[z * room : (z + 1) * room]
    send_ref[pl.ds(room, PLANES, room + 1), :] = notes
    for copy in tables:
        copy.wait()


def seats(notes, z, place, room):
    return onehot(iota((place, room), 0) == notes[z : z + 1, :room].astype(jnp.int32) - 1)


def turn_kernel(got_ref, send_ref):
    room = got_ref.shape[0] // PLANES - 1
    place = send_ref.shape[0] // (PLANES + 1)
    lanes = got_ref.shape[1]
    notes = got_ref[pl.ds(room, PLANES, room + 1), :]
    turned = jnp.concatenate([notes, jnp.zeros((lanes - PLANES, lanes), F32)], axis=0).T
    slots = turned[room : 2 * room] + pltpu.roll(turned[2 * room : 3 * room], PLANES, 1)
    lane = iota((room, lanes), 1)
    picks, parts = [], []
    for z in range(PLANES):
        pick = seats(notes, z, place, room)
        hi, lo = pieces(got_ref[pl.ds(z * (room + 1), room), :], 2)
        send_ref[pl.ds(z, place, PLANES + 1), :] = contract(
            jnp.concatenate([pick, pick], axis=1), jnp.concatenate([hi, lo], axis=0), 1, 0
        )
        picks.append(pick)
        mine = (lane == z) | (lane == PLANES + z)
        parts.append(jnp.where(mine, slots, F32(0.0)).astype(BF16))
    passed = contract(jnp.concatenate(picks, axis=1), jnp.concatenate(parts, axis=0), 1, 0)
    full = jnp.max(notes[:, lanes - 1 :], axis=0, keepdims=True)
    passed = jnp.where(iota((place, lanes), 1) == lanes - 1, full, passed)
    send_ref[pl.ds(PLANES, place, PLANES + 1), :] = passed


def turn_back_kernel(got_ref, back_ref, send_ref):
    room = got_ref.shape[0] // PLANES - 1
    place = back_ref.shape[0] // PLANES
    notes = got_ref[pl.ds(room, PLANES, room + 1), :]
    for z in range(PLANES):
        pick = seats(notes, z, place, room)
        hi, lo = pieces(back_ref[pl.ds(z, place, PLANES), :], 2)
        send_ref[pl.ds(z * room, room), :] = contract(
            jnp.concatenate([pick, pick], axis=0), jnp.concatenate([hi, lo], axis=0), 0, 0
        )


def merge_kernel(got_ref, table_ref, merged_ref, reply_ref, full_ref):
    width, cells = merged_ref.shape
    devices = reply_ref.shape[0]
    place = devices // PLANES
    rows = jnp.concatenate(
        [got_ref[pl.ds(z, place, PLANES + 1), :] for z in range(PLANES)], axis=0
    )
    slots = got_ref[pl.ds(PLANES, place, PLANES + 1), :].astype(jnp.int32) - 1
    full_ref[0] = jnp.max(slots[:, slots.shape[1] - 1 :]) + 1
    lane = iota((place, cells), 1)
    first, second = (
        jnp.concatenate(
            [onehot(lane == slots[:, k + z : k + z + 1]) for z in range(PLANES)], axis=0
        )
        for k in (0, PLANES)
    )
    field, frac = table_ref[:width, :], table_ref[width:, :]
    merged = frac * from_rows(rows, first, second) + (1.0 - frac) * field
    merged_ref[...] = merged
    masks = jnp.concatenate([first, first, second, second], axis=1)
    rows = contract(masks, side_by_side(merged), 1, 1)
    for z in range(PLANES):
        reply_ref[pl.ds(z, place, PLANES), :] = rows[z * place : (z + 1) * place]


def spread_kernel(count_ref, back_ref, first_ref, second_ref, cell_of_ref, scaled_ref, out_ref):
    width, patches = scaled_ref.shape
    merged = from_rows(back_ref[...], first_ref[...], second_ref[...])
    parts = contract(jnp.concatenate(pieces(merged, 2), axis=0), cell_of_ref[...], 1, 0)
    picked = parts[:width] + parts[width:]
    alive = iota((1, patches), 1) < count_ref[0]
    out_ref[...] = jnp.where(alive, scaled_ref[...] - picked, F32(0.0))


PARAMS = pltpu.CompilerParams(vmem_limit_bytes=12 << 20)
VMEM = pl.BlockSpec(memory_space=pltpu.VMEM)
HBM = pl.BlockSpec(memory_space=pltpu.HBM)
SMEM = pl.BlockSpec(memory_space=pltpu.SMEM)


def exchange(x, axis, groups):
    return lax.all_to_all(
        x, axis, split_axis=0, concat_axis=0, tiled=True, axis_index_groups=groups
    )


def pipeline(
    room,
    flux,
    patch_pft,
    patch_wt,
    patch_col,
    col_wt,
    col_lu,
    lu_wt,
    lu_grid,
    cell_target,
    patch_count,
    pft_scale,
    cpl_frac,
    cpl_field,
):
    devices = lax.axis_size("clump") * lax.axis_size("grp")
    patches, width = flux.shape[1:]
    cells = cell_target.shape[1]
    shape = jax.ShapeDtypeStruct
    lanes = 2 * width
    place = devices // PLANES
    columns = lax.axis_size("clump") // PLANES
    along = [[z * columns + i for z in range(PLANES)] for i in range(columns)]
    across = [[z * place + i for i in range(place)] for z in range(PLANES)]
    send, table, scaled, cell_of, first, second = pl.pallas_call(
        functools.partial(gather_kernel, devices),
        out_shape=(
            shape((PLANES * (room + 1), lanes), F32),
            shape((width + 1, cells), F32),
            shape((width, patches), F32),
            shape((cells, patches), BF16),
            shape((PLANES * room, cells), BF16),
            shape((PLANES * room, cells), BF16),
        ),
        in_specs=[SMEM] + [HBM] * 12,
        out_specs=(VMEM,) * 6,
        scratch_shapes=[
            pltpu.VMEM(col_lu.shape, jnp.int32),
            pltpu.VMEM(lu_wt.shape, F32),
            pltpu.VMEM(lu_grid.shape, jnp.int32),
            pltpu.VMEM(col_wt.shape, F32),
            pltpu.VMEM(patch_col.shape, jnp.int32),
            pltpu.VMEM(patch_pft.shape, jnp.int32),
            pltpu.VMEM(pft_scale.shape, F32),
            pltpu.VMEM(patch_wt.shape, F32),
            pltpu.VMEM(cell_target.shape, jnp.int32),
            pltpu.VMEM((width, patches), F32),
            pltpu.SemaphoreType.DMA((12,)),
        ],
        compiler_params=PARAMS,
        name="gather_cells",
    )(
        patch_count,
        *(
            pltpu.with_memory_space_constraint(x, pltpu.HBM)
            for x in (
                flux[0].T,
                patch_pft,
                patch_wt,
                patch_col,
                col_wt,
                col_lu,
                lu_wt,
                lu_grid,
                cell_target,
                pft_scale,
                cpl_field.T,
                cpl_frac.reshape(1, cells),
            )
        ),
    )
    noted = exchange(send.reshape(PLANES, 1, (room + 1) * lanes), "clump", along)
    noted = noted.reshape(PLANES * (room + 1), lanes)
    send = pl.pallas_call(
        turn_kernel,
        out_shape=shape((place * (PLANES + 1), lanes), F32),
        in_specs=[VMEM],
        out_specs=VMEM,
        compiler_params=PARAMS,
        name="turn_rows",
    )(noted)
    got = exchange(send.reshape(place, 1, (PLANES + 1) * lanes), AXES, across)
    merged, reply, full = pl.pallas_call(
        merge_kernel,
        out_shape=(
            shape((width, cells), F32),
            shape((devices, lanes), F32),
            shape((1,), jnp.int32),
        ),
        in_specs=[VMEM] * 2,
        out_specs=(VMEM, VMEM, SMEM),
        compiler_params=PARAMS,
        name="merge_cells",
    )(got.reshape(place * (PLANES + 1), lanes), table)
    back = exchange(reply.reshape(place, 1, PLANES * lanes), AXES, across)
    back = pl.pallas_call(
        turn_back_kernel,
        out_shape=shape((PLANES * room, lanes), F32),
        in_specs=[VMEM] * 2,
        out_specs=VMEM,
        compiler_params=PARAMS,
        name="turn_back",
    )(noted, back.reshape(devices, lanes))
    back = exchange(back.reshape(PLANES, 1, room * lanes), "clump", along)
    back = back.reshape(PLANES * room, lanes)
    anomaly = pl.pallas_call(
        spread_kernel,
        out_shape=shape((width, patches), F32),
        in_specs=[SMEM] + [VMEM] * 5,
        out_specs=VMEM,
        compiler_params=PARAMS,
        name="spread_cells",
    )(patch_count, back, first, second, cell_of, scaled)
    return merged, anomaly, full[0]


def per_device(*args):
    devices = lax.axis_size("clump") * lax.axis_size("grp")
    most = devices // PLANES

    def again(state):
        merged, anomaly, _ = pipeline(most, *args)
        return merged, anomaly, jnp.int32(0)

    merged, anomaly, _ = lax.while_loop(
        lambda state: state[2] > 0, again, pipeline(most // 2, *args)
    )
    return merged.T, anomaly.T[None]


def solution(mesh):
    rows = P(AXES, None)
    return jax.shard_map(
        per_device,
        mesh=mesh,
        in_specs=(
            P(AXES, None, None),
            rows,
            rows,
            rows,
            rows,
            rows,
            rows,
            rows,
            rows,
            P(AXES),
            P(),
            P(AXES),
            rows,
        ),
        out_specs=(rows, P(AXES, None, None)),
        check_vma=False,
    )
```

```python
import functools

import jax
import jax.numpy as jnp
from jax import lax
from jax.experimental import pallas as pl
from jax.experimental.pallas import tpu as pltpu
from jax.sharding import PartitionSpec as P

F32 = jnp.float32
BF16 = jnp.bfloat16
AXES = ("clump", "grp")
PLANES = 16


def pieces(x, count):
    parts = []
    for _ in range(count):
        part = x.astype(BF16)
        parts.append(part)
        x = x - part.astype(F32)
    return parts


def contract(a, b, da, db):
    return lax.dot_general(a, b, (((da,), (db,)), ((), ())), preferred_element_type=F32)


def onehot(mask):
    return jnp.where(mask, F32(1.0), F32(0.0)).astype(BF16)


def iota(shape, dim):
    return lax.broadcasted_iota(jnp.int32, shape, dim)


def cell_rows(target, cells, devices):
    place = devices // PLANES
    owner = target // cells
    across = jnp.broadcast_to(owner, (cells, cells)).astype(F32)
    down = across.T
    base = jnp.broadcast_to(owner - owner % place, (cells, cells)).astype(F32)
    earlier = (down == across) & (iota((cells, cells), 0) < iota((cells, cells), 1))
    rank = jnp.max(jnp.where(earlier, F32(1.0), F32(0.0)), axis=0, keepdims=True)
    below = (down < across) & (down >= base)
    row = jnp.sum(jnp.where(below, F32(0.5), F32(0.0)), axis=0, keepdims=True)
    return owner // place, owner % place, rank > 0.5, row.astype(jnp.int32)


def side_by_side(x):
    hi, lo = pieces(x, 2)
    both = jnp.concatenate([hi, lo], axis=1)
    zero = jnp.zeros_like(both)
    return jnp.concatenate(
        [jnp.concatenate([both, zero], axis=1), jnp.concatenate([zero, both], axis=1)], axis=0
    )


def from_rows(rows, first, second):
    width = rows.shape[1] // 2
    hi = rows.astype(BF16).astype(F32)
    lo = rows - hi
    left = iota(rows.shape, 1) < width
    one = jnp.where(left, hi, pltpu.roll(lo, width, 1)).astype(BF16)
    two = jnp.where(left, pltpu.roll(hi, width, 1), lo).astype(BF16)
    both = contract(
        jnp.concatenate([one, two], axis=0), jnp.concatenate([first, second], axis=0), 0, 0
    )
    return both[:width] + both[width:]


def gather_kernel(
    devices,
    count_ref,
    flux_ref,
    pft_ref,
    wt_ref,
    col_ref,
    col_wt_ref,
    col_lu_ref,
    lu_wt_ref,
    lu_grid_ref,
    target_ref,
    scale_ref,
    field_ref,
    frac_ref,
    send_ref,
    table_ref,
    scaled_ref,
    cell_of_ref,
    first_ref,
    second_ref,
    *scratch,
):
    held, sems = scratch[:-1], scratch[-1]
    given = (
        col_lu_ref,
        lu_wt_ref,
        lu_grid_ref,
        col_wt_ref,
        col_ref,
        pft_ref,
        scale_ref,
        wt_ref,
        target_ref,
        flux_ref,
    )
    copies = [
        pltpu.make_async_copy(src, dst, sems.at[i]) for i, (src, dst) in enumerate(zip(given, held))
    ]
    tables = [
        pltpu.make_async_copy(field_ref, table_ref.at[pl.ds(0, field_ref.shape[0])], sems.at[10]),
        pltpu.make_async_copy(frac_ref, table_ref.at[pl.ds(field_ref.shape[0], 1)], sems.at[11]),
    ]
    for copy in copies + tables:
        copy.start()
    (
        col_lu_ref,
        lu_wt_ref,
        lu_grid_ref,
        col_wt_ref,
        col_ref,
        pft_ref,
        scale_ref,
        wt_ref,
        target_ref,
        flux_ref,
    ) = held
    for copy in copies[:9]:
        copy.wait()
    width, patches = flux_ref.shape
    cells = target_ref.shape[1]
    room = send_ref.shape[0] // PLANES - 1
    lanes = send_ref.shape[1]
    columns = col_wt_ref.shape[1]
    units = lu_wt_ref.shape[1]
    types = scale_ref.shape[0]

    unit_table = jnp.concatenate(
        pieces(lu_wt_ref[...], 3)
        + [lu_grid_ref[...].astype(F32).astype(BF16), jnp.zeros((12, units), BF16)],
        axis=0,
    )
    unit_of = onehot(iota((units, columns), 0) == col_lu_ref[...])
    picked = contract(unit_table, unit_of, 1, 0)
    col_weight = col_wt_ref[...] * (picked[0:1] + picked[1:2] + picked[2:3])
    col_table = jnp.concatenate(
        pieces(col_weight, 3) + [picked[3:4].astype(BF16), jnp.zeros((12, columns), BF16)], axis=0
    )
    parts = []
    span = patches // 4
    for block in range(4):
        start = block * span
        low = max(start // 4, start - columns) // 128 * 128
        high = min(start + span, columns // 2 + start // 4 + span // 4, columns)
        high = -(-high // 128) * 128
        here = iota((high - low, span), 0) + low == col_ref[:, start : start + span]
        parts.append(contract(col_table[:, low:high], onehot(here), 1, 0))
    picked = jnp.concatenate(parts, axis=1)
    alive = iota((1, patches), 1) < count_ref[0]
    weight = jnp.where(
        alive, wt_ref[...] * (picked[0:1] + picked[1:2] + picked[2:3]), F32(0.0)
    )
    home = picked[3:4].astype(jnp.int32)

    type_of = onehot(iota((types, patches), 0) == pft_ref[...])
    scale_parts = jnp.concatenate(pieces(scale_ref[...], 3), axis=0)
    factor = contract(scale_parts, jnp.concatenate([type_of] * 3, axis=0), 0, 0)
    copies[9].wait()
    scaled = flux_ref[...] * factor
    scaled_ref[...] = jnp.where(alive, scaled, F32(0.0))

    cell_of = onehot((iota((cells, patches), 0) == home) & alive)
    cell_of_ref[...] = cell_of
    terms = jnp.concatenate([scaled * weight, weight, jnp.zeros((15, patches), F32)], axis=0)
    sums = [contract(part, cell_of, 1, 1) for part in pieces(terms, 2)]
    total = sums[0] + sums[1]
    mean = total[:width] / jnp.maximum(total[width : width + 1], 1.0)

    target = target_ref[...]
    plane, place, second, row = cell_rows(target, cells, devices)
    hit = iota((PLANES * room, cells), 0) == plane * room + row
    one, two = onehot(hit & jnp.logical_not(second)), onehot(hit & second)
    first_ref[...] = one
    second_ref[...] = two
    rows = contract(jnp.concatenate([one, one, two, two], axis=1), side_by_side(mean), 1, 1)

    in_plane = iota((PLANES, cells), 0) == plane
    slot = (target % cells + 1).astype(F32)
    seat = jnp.where(second, F32(0.0), (place + 1).astype(F32))
    left = jnp.concatenate(
        [jnp.where(in_plane, seat, F32(0.0)), jnp.where(in_plane, slot, F32(0.0))], axis=1
    ).astype(BF16)
    lane = iota((lanes, cells), 0)
    right = jnp.concatenate(
        [onehot(lane == row), onehot(lane == row + jnp.where(second, 2 * room, room))], axis=1
    )
    notes = contract(left, right, 1, 1)
    full = jnp.where(jnp.max(row, axis=1, keepdims=True) < room, F32(0.0), F32(1.0))
    notes = jnp.where(iota((PLANES, lanes), 1) == lanes - 1, full, notes)
    for z in range(PLANES):
        send_ref[pl.ds(z * (room + 1), room), :] = rows[z * room : (z + 1) * room]
    send_ref[pl.ds(room, PLANES, room + 1), :] = notes
    for copy in tables:
        copy.wait()


def seats(notes, z, place, room):
    return onehot(iota((place, room), 0) == notes[z : z + 1, :room].astype(jnp.int32) - 1)


def turn_kernel(got_ref, send_ref):
    room = got_ref.shape[0] // PLANES - 1
    place = send_ref.shape[0] // (PLANES + 1)
    lanes = got_ref.shape[1]
    notes = got_ref[pl.ds(room, PLANES, room + 1), :]
    turned = jnp.concatenate([notes, jnp.zeros((lanes - PLANES, lanes), F32)], axis=0).T
    slots = turned[room : 2 * room] + pltpu.roll(turned[2 * room : 3 * room], PLANES, 1)
    lane = iota((room, lanes), 1)
    picks, parts = [], []
    for z in range(PLANES):
        pick = seats(notes, z, place, room)
        hi, lo = pieces(got_ref[pl.ds(z * (room + 1), room), :], 2)
        send_ref[pl.ds(z, place, PLANES + 1), :] = contract(
            jnp.concatenate([pick, pick], axis=1), jnp.concatenate([hi, lo], axis=0), 1, 0
        )
        picks.append(pick)
        mine = (lane == z) | (lane == PLANES + z)
        parts.append(jnp.where(mine, slots, F32(0.0)).astype(BF16))
    passed = contract(jnp.concatenate(picks, axis=1), jnp.concatenate(parts, axis=0), 1, 0)
    full = jnp.max(notes[:, lanes - 1 :], axis=0, keepdims=True)
    passed = jnp.where(iota((place, lanes), 1) == lanes - 1, full, passed)
    send_ref[pl.ds(PLANES, place, PLANES + 1), :] = passed


def turn_back_kernel(got_ref, back_ref, send_ref):
    room = got_ref.shape[0] // PLANES - 1
    place = back_ref.shape[0] // PLANES
    notes = got_ref[pl.ds(room, PLANES, room + 1), :]
    for z in range(PLANES):
        pick = seats(notes, z, place, room)
        hi, lo = pieces(back_ref[pl.ds(z, place, PLANES), :], 2)
        send_ref[pl.ds(z * room, room), :] = contract(
            jnp.concatenate([pick, pick], axis=0), jnp.concatenate([hi, lo], axis=0), 0, 0
        )


def merge_kernel(got_ref, table_ref, merged_ref, reply_ref, full_ref, held_ref, flag_ref, sems):
    width, cells = held_ref.shape
    devices = reply_ref.shape[0]
    place = devices // PLANES
    rows = jnp.concatenate(
        [got_ref[pl.ds(z, place, PLANES + 1), :] for z in range(PLANES)], axis=0
    )
    slots = got_ref[pl.ds(PLANES, place, PLANES + 1), :].astype(jnp.int32) - 1
    flag_ref[0] = jnp.max(slots[:, slots.shape[1] - 1 :]) + 1
    copies = (
        pltpu.make_async_copy(flag_ref, full_ref, sems.at[0]),
        pltpu.make_async_copy(held_ref, merged_ref, sems.at[1]),
    )
    copies[0].start()
    lane = iota((place, cells), 1)
    first, second = (
        jnp.concatenate(
            [onehot(lane == slots[:, k + z : k + z + 1]) for z in range(PLANES)], axis=0
        )
        for k in (0, PLANES)
    )
    field, frac = table_ref[:width, :], table_ref[width:, :]
    merged = frac * from_rows(rows, first, second) + (1.0 - frac) * field
    held_ref[...] = merged
    copies[1].start()
    masks = jnp.concatenate([first, first, second, second], axis=1)
    rows = contract(masks, side_by_side(merged), 1, 1)
    for z in range(PLANES):
        reply_ref[pl.ds(z, place, PLANES), :] = rows[z * place : (z + 1) * place]
    for copy in copies:
        copy.wait()


def spread_kernel(
    back_ref, first_ref, second_ref, cell_of_ref, scaled_ref, out_ref, held_ref, sems
):
    width, patches = scaled_ref.shape
    merged = from_rows(back_ref[...], first_ref[...], second_ref[...])
    both = jnp.concatenate(pieces(merged, 2), axis=0)
    chunk = patches // 4
    copies = []
    for i in range(4):
        here = pl.ds(i * chunk, chunk)
        parts = contract(both, cell_of_ref[:, here], 1, 0)
        held_ref[:, here] = scaled_ref[:, here] - (parts[:width] + parts[width:])
        copies.append(
            pltpu.make_async_copy(held_ref.at[:, here], out_ref.at[:, here], sems.at[i])
        )
        copies[i].start()
    for copy in copies:
        copy.wait()


PARAMS = pltpu.CompilerParams(vmem_limit_bytes=12 << 20)
VMEM = pl.BlockSpec(memory_space=pltpu.VMEM)
HBM = pl.BlockSpec(memory_space=pltpu.HBM)
SMEM = pl.BlockSpec(memory_space=pltpu.SMEM)
ANY = pl.BlockSpec(memory_space=pl.ANY)


def exchange(x, axis, groups):
    return lax.all_to_all(
        x, axis, split_axis=0, concat_axis=0, tiled=True, axis_index_groups=groups
    )


def pipeline(
    room,
    flux,
    patch_pft,
    patch_wt,
    patch_col,
    col_wt,
    col_lu,
    lu_wt,
    lu_grid,
    cell_target,
    patch_count,
    pft_scale,
    cpl_frac,
    cpl_field,
):
    devices = lax.axis_size("clump") * lax.axis_size("grp")
    patches, width = flux.shape[1:]
    cells = cell_target.shape[1]
    shape = jax.ShapeDtypeStruct
    lanes = 2 * width
    place = devices // PLANES
    columns = lax.axis_size("clump") // PLANES
    along = [[z * columns + i for z in range(PLANES)] for i in range(columns)]
    across = [[z * place + i for i in range(place)] for z in range(PLANES)]
    send, table, scaled, cell_of, first, second = pl.pallas_call(
        functools.partial(gather_kernel, devices),
        out_shape=(
            shape((PLANES * (room + 1), lanes), F32),
            shape((width + 1, cells), F32),
            shape((width, patches), F32),
            shape((cells, patches), BF16),
            shape((PLANES * room, cells), BF16),
            shape((PLANES * room, cells), BF16),
        ),
        in_specs=[SMEM] + [HBM] * 12,
        out_specs=(VMEM,) * 6,
        scratch_shapes=[
            pltpu.VMEM(col_lu.shape, jnp.int32),
            pltpu.VMEM(lu_wt.shape, F32),
            pltpu.VMEM(lu_grid.shape, jnp.int32),
            pltpu.VMEM(col_wt.shape, F32),
            pltpu.VMEM(patch_col.shape, jnp.int32),
            pltpu.VMEM(patch_pft.shape, jnp.int32),
            pltpu.VMEM(pft_scale.shape, F32),
            pltpu.VMEM(patch_wt.shape, F32),
            pltpu.VMEM(cell_target.shape, jnp.int32),
            pltpu.VMEM((width, patches), F32),
            pltpu.SemaphoreType.DMA((12,)),
        ],
        compiler_params=PARAMS,
        name="gather_cells",
    )(
        patch_count,
        *(
            pltpu.with_memory_space_constraint(x, pltpu.HBM)
            for x in (
                flux[0].T,
                patch_pft,
                patch_wt,
                patch_col,
                col_wt,
                col_lu,
                lu_wt,
                lu_grid,
                cell_target,
                pft_scale,
                cpl_field.T,
                cpl_frac.reshape(1, cells),
            )
        ),
    )
    noted = exchange(send.reshape(PLANES, 1, (room + 1) * lanes), "clump", along)
    noted = noted.reshape(PLANES * (room + 1), lanes)
    send = pl.pallas_call(
        turn_kernel,
        out_shape=shape((place * (PLANES + 1), lanes), F32),
        in_specs=[VMEM],
        out_specs=VMEM,
        compiler_params=PARAMS,
        name="turn_rows",
    )(noted)
    got = exchange(send.reshape(place, 1, (PLANES + 1) * lanes), AXES, across)
    merged, reply, full = pl.pallas_call(
        merge_kernel,
        out_shape=(
            shape((width, cells), F32),
            shape((devices, lanes), F32),
            shape((1,), jnp.int32),
        ),
        in_specs=[VMEM] * 2,
        out_specs=(ANY, VMEM, ANY),
        scratch_shapes=[
            pltpu.VMEM((width, cells), F32),
            pltpu.SMEM((1,), jnp.int32),
            pltpu.SemaphoreType.DMA((2,)),
        ],
        compiler_params=PARAMS,
        name="merge_cells",
    )(got.reshape(place * (PLANES + 1), lanes), table)
    back = exchange(reply.reshape(place, 1, PLANES * lanes), AXES, across)
    back = pl.pallas_call(
        turn_back_kernel,
        out_shape=shape((PLANES * room, lanes), F32),
        in_specs=[VMEM] * 2,
        out_specs=VMEM,
        compiler_params=PARAMS,
        name="turn_back",
    )(noted, back.reshape(devices, lanes))
    back = exchange(back.reshape(PLANES, 1, room * lanes), "clump", along)
    back = back.reshape(PLANES * room, lanes)
    anomaly = pl.pallas_call(
        spread_kernel,
        out_shape=shape((width, patches), F32),
        in_specs=[VMEM] * 5,
        out_specs=ANY,
        scratch_shapes=[
            pltpu.VMEM((width, patches), F32),
            pltpu.SemaphoreType.DMA((4,)),
        ],
        compiler_params=PARAMS,
        name="spread_cells",
    )(back, first, second, cell_of, scaled)
    return merged, anomaly, full[0]


def per_device(*args):
    devices = lax.axis_size("clump") * lax.axis_size("grp")
    most = devices // PLANES

    def again(state):
        merged, anomaly, _ = pipeline(most, *args)
        return merged, anomaly, jnp.int32(0)

    merged, anomaly, _ = lax.while_loop(
        lambda state: state[2] > 0, again, pipeline(most // 2, *args)
    )
    return merged.T, anomaly.T[None]


def solution(mesh):
    rows = P(AXES, None)
    return jax.shard_map(
        per_device,
        mesh=mesh,
        in_specs=(
            P(AXES, None, None),
            rows,
            rows,
            rows,
            rows,
            rows,
            rows,
            rows,
            rows,
            P(AXES),
            P(),
            P(AXES),
            rows,
        ),
        out_specs=(rows, P(AXES, None, None)),
        check_vma=False,
    )
```

```python
import functools

import jax
import jax.numpy as jnp
from jax import lax
from jax.experimental import pallas as pl
from jax.experimental.pallas import tpu as pltpu
from jax.sharding import PartitionSpec as P

F32 = jnp.float32
BF16 = jnp.bfloat16
AXES = ("clump", "grp")
PLANES = 16


def pieces(x, count):
    parts = []
    for _ in range(count):
        part = x.astype(BF16)
        parts.append(part)
        x = x - part.astype(F32)
    return parts


def contract(a, b, da, db):
    return lax.dot_general(a, b, (((da,), (db,)), ((), ())), preferred_element_type=F32)


def onehot(mask):
    return jnp.where(mask, F32(1.0), F32(0.0)).astype(BF16)


def iota(shape, dim):
    return lax.broadcasted_iota(jnp.int32, shape, dim)


def cell_rows(target, cells, devices):
    place = devices // PLANES
    owner = target // cells
    across = jnp.broadcast_to(owner, (cells, cells)).astype(F32)
    down = across.T
    base = jnp.broadcast_to(owner - owner % place, (cells, cells)).astype(F32)
    earlier = (down == across) & (iota((cells, cells), 0) < iota((cells, cells), 1))
    rank = jnp.max(jnp.where(earlier, F32(1.0), F32(0.0)), axis=0, keepdims=True)
    below = (down < across) & (down >= base)
    row = jnp.sum(jnp.where(below, F32(0.5), F32(0.0)), axis=0, keepdims=True)
    return owner // place, owner % place, rank > 0.5, row.astype(jnp.int32)


def side_by_side(x):
    hi, lo = pieces(x, 2)
    both = jnp.concatenate([hi, lo], axis=1)
    zero = jnp.zeros_like(both)
    return jnp.concatenate(
        [jnp.concatenate([both, zero], axis=1), jnp.concatenate([zero, both], axis=1)], axis=0
    )


def from_rows(rows, first, second):
    width = rows.shape[1] // 2
    hi = rows.astype(BF16).astype(F32)
    lo = rows - hi
    left = iota(rows.shape, 1) < width
    one = jnp.where(left, hi, pltpu.roll(lo, width, 1)).astype(BF16)
    two = jnp.where(left, pltpu.roll(hi, width, 1), lo).astype(BF16)
    both = contract(
        jnp.concatenate([one, two], axis=0), jnp.concatenate([first, second], axis=0), 0, 0
    )
    return both[:width] + both[width:]


def gather_kernel(
    devices,
    count_ref,
    flux_ref,
    pft_ref,
    wt_ref,
    col_ref,
    col_wt_ref,
    col_lu_ref,
    lu_wt_ref,
    lu_grid_ref,
    target_ref,
    scale_ref,
    field_ref,
    frac_ref,
    send_ref,
    table_ref,
    scaled_ref,
    cell_of_ref,
    first_ref,
    second_ref,
    *scratch,
):
    held, sems = scratch[:-1], scratch[-1]
    given = (
        col_lu_ref,
        lu_wt_ref,
        lu_grid_ref,
        col_wt_ref,
        col_ref,
        pft_ref,
        scale_ref,
        wt_ref,
        target_ref,
        flux_ref,
    )
    copies = [
        pltpu.make_async_copy(src, dst, sems.at[i]) for i, (src, dst) in enumerate(zip(given, held))
    ]
    tables = [
        pltpu.make_async_copy(field_ref, table_ref.at[pl.ds(0, field_ref.shape[0])], sems.at[10]),
        pltpu.make_async_copy(frac_ref, table_ref.at[pl.ds(field_ref.shape[0], 1)], sems.at[11]),
    ]
    for copy in copies + tables:
        copy.start()
    (
        col_lu_ref,
        lu_wt_ref,
        lu_grid_ref,
        col_wt_ref,
        col_ref,
        pft_ref,
        scale_ref,
        wt_ref,
        target_ref,
        flux_ref,
    ) = held
    for copy in copies[:9]:
        copy.wait()
    width, patches = flux_ref.shape
    cells = target_ref.shape[1]
    room = send_ref.shape[0] // PLANES - 1
    lanes = send_ref.shape[1]
    columns = col_wt_ref.shape[1]
    units = lu_wt_ref.shape[1]
    types = scale_ref.shape[0]

    unit_table = jnp.concatenate(
        pieces(lu_wt_ref[...], 3)
        + [lu_grid_ref[...].astype(F32).astype(BF16), jnp.zeros((12, units), BF16)],
        axis=0,
    )
    unit_of = onehot(iota((units, columns), 0) == col_lu_ref[...])
    picked = contract(unit_table, unit_of, 1, 0)
    col_weight = col_wt_ref[...] * (picked[0:1] + picked[1:2] + picked[2:3])
    col_table = jnp.concatenate(
        pieces(col_weight, 3) + [picked[3:4].astype(BF16), jnp.zeros((12, columns), BF16)], axis=0
    )
    parts = []
    span = patches // 4
    for block in range(4):
        start = block * span
        low = max(start // 4, start - columns) // 128 * 128
        high = min(start + span, columns // 2 + start // 4 + span // 4, columns)
        high = -(-high // 128) * 128
        here = iota((high - low, span), 0) + low == col_ref[:, start : start + span]
        parts.append(contract(col_table[:, low:high], onehot(here), 1, 0))
    picked = jnp.concatenate(parts, axis=1)
    alive = iota((1, patches), 1) < count_ref[0]
    weight = jnp.where(
        alive, wt_ref[...] * (picked[0:1] + picked[1:2] + picked[2:3]), F32(0.0)
    )
    home = picked[3:4].astype(jnp.int32)

    type_of = onehot(iota((types, patches), 0) == pft_ref[...])
    scale_parts = jnp.concatenate(pieces(scale_ref[...], 3), axis=0)
    factor = contract(scale_parts, jnp.concatenate([type_of] * 3, axis=0), 0, 0)
    copies[9].wait()
    scaled = flux_ref[...] * factor
    scaled_ref[...] = jnp.where(alive, scaled, F32(0.0))

    cell_of = onehot((iota((cells, patches), 0) == home) & alive)
    cell_of_ref[...] = cell_of
    terms = jnp.concatenate([scaled * weight, weight, jnp.zeros((15, patches), F32)], axis=0)
    sums = [contract(part, cell_of, 1, 1) for part in pieces(terms, 2)]
    total = sums[0] + sums[1]
    mean = total[:width] / jnp.maximum(total[width : width + 1], 1.0)

    target = target_ref[...]
    plane, place, second, row = cell_rows(target, cells, devices)
    hit = iota((PLANES * room, cells), 0) == plane * room + row
    one, two = onehot(hit & jnp.logical_not(second)), onehot(hit & second)
    first_ref[...] = one
    second_ref[...] = two
    rows = contract(jnp.concatenate([one, one, two, two], axis=1), side_by_side(mean), 1, 1)

    in_plane = iota((PLANES, cells), 0) == plane
    slot = (target % cells + 1).astype(F32)
    seat = jnp.where(second, F32(0.0), (place + 1).astype(F32))
    left = jnp.concatenate(
        [jnp.where(in_plane, seat, F32(0.0)), jnp.where(in_plane, slot, F32(0.0))], axis=1
    ).astype(BF16)
    lane = iota((lanes, cells), 0)
    right = jnp.concatenate(
        [onehot(lane == row), onehot(lane == row + jnp.where(second, 2 * room, room))], axis=1
    )
    notes = contract(left, right, 1, 1)
    full = jnp.where(jnp.max(row, axis=1, keepdims=True) < room, F32(0.0), F32(1.0))
    notes = jnp.where(iota((PLANES, lanes), 1) == lanes - 1, full, notes)
    for z in range(PLANES):
        send_ref[pl.ds(z * (room + 1), room), :] = rows[z * room : (z + 1) * room]
    send_ref[pl.ds(room, PLANES, room + 1), :] = notes
    for copy in tables:
        copy.wait()


def seats(notes, z, place, room):
    return onehot(iota((place, room), 0) == notes[z : z + 1, :room].astype(jnp.int32) - 1)


def turn_kernel(got_ref, send_ref):
    room = got_ref.shape[0] // PLANES - 1
    place = send_ref.shape[0] // (PLANES + 1)
    lanes = got_ref.shape[1]
    notes = got_ref[pl.ds(room, PLANES, room + 1), :]
    turned = jnp.concatenate([notes, jnp.zeros((lanes - PLANES, lanes), F32)], axis=0).T
    slots = turned[room : 2 * room] + pltpu.roll(turned[2 * room : 3 * room], PLANES, 1)
    lane = iota((room, lanes), 1)
    picks, parts = [], []
    for z in range(PLANES):
        pick = seats(notes, z, place, room)
        hi, lo = pieces(got_ref[pl.ds(z * (room + 1), room), :], 2)
        send_ref[pl.ds(z, place, PLANES + 1), :] = contract(
            jnp.concatenate([pick, pick], axis=1), jnp.concatenate([hi, lo], axis=0), 1, 0
        )
        picks.append(pick)
        mine = (lane == z) | (lane == PLANES + z)
        parts.append(jnp.where(mine, slots, F32(0.0)).astype(BF16))
    passed = contract(jnp.concatenate(picks, axis=1), jnp.concatenate(parts, axis=0), 1, 0)
    full = jnp.max(notes[:, lanes - 1 :], axis=0, keepdims=True)
    passed = jnp.where(iota((place, lanes), 1) == lanes - 1, full, passed)
    send_ref[pl.ds(PLANES, place, PLANES + 1), :] = passed


def turn_back_kernel(got_ref, back_ref, send_ref):
    room = got_ref.shape[0] // PLANES - 1
    place = back_ref.shape[0] // PLANES
    notes = got_ref[pl.ds(room, PLANES, room + 1), :]
    for z in range(PLANES):
        pick = seats(notes, z, place, room)
        hi, lo = pieces(back_ref[pl.ds(z, place, PLANES), :], 2)
        send_ref[pl.ds(z * room, room), :] = contract(
            jnp.concatenate([pick, pick], axis=0), jnp.concatenate([hi, lo], axis=0), 0, 0
        )


def merge_kernel(got_ref, table_ref, merged_ref, reply_ref, full_ref):
    width, cells = merged_ref.shape
    devices = reply_ref.shape[0]
    place = devices // PLANES
    rows = jnp.concatenate(
        [got_ref[pl.ds(z, place, PLANES + 1), :] for z in range(PLANES)], axis=0
    )
    slots = got_ref[pl.ds(PLANES, place, PLANES + 1), :].astype(jnp.int32) - 1
    full_ref[...] = jnp.broadcast_to(jnp.max(slots, axis=0, keepdims=True), full_ref.shape)
    lane = iota((place, cells), 1)
    first, second = (
        jnp.concatenate(
            [onehot(lane == slots[:, k + z : k + z + 1]) for z in range(PLANES)], axis=0
        )
        for k in (0, PLANES)
    )
    field, frac = table_ref[:width, :], table_ref[width:, :]
    merged = frac * from_rows(rows, first, second) + (1.0 - frac) * field
    merged_ref[...] = merged
    masks = jnp.concatenate([first, first, second, second], axis=1)
    rows = contract(masks, side_by_side(merged), 1, 1)
    for z in range(PLANES):
        reply_ref[pl.ds(z, place, PLANES), :] = rows[z * place : (z + 1) * place]


def spread_kernel(
    back_ref,
    first_ref,
    second_ref,
    cell_of_ref,
    scaled_ref,
    mine_ref,
    notes_ref,
    out_ref,
    merged_ref,
    full_ref,
    held_ref,
    flag_ref,
    sems,
):
    width, patches = scaled_ref.shape
    kept = pltpu.make_async_copy(mine_ref, merged_ref, sems.at[4])
    kept.start()
    merged = from_rows(back_ref[...], first_ref[...], second_ref[...])
    both = jnp.concatenate(pieces(merged, 2), axis=0)
    chunk = patches // 4
    copies = []
    for i in range(4):
        here = pl.ds(i * chunk, chunk)
        parts = contract(both, cell_of_ref[:, here], 1, 0)
        held_ref[:, here] = scaled_ref[:, here] - (parts[:width] + parts[width:])
        copies.append(
            pltpu.make_async_copy(held_ref.at[:, here], out_ref.at[:, here], sems.at[i])
        )
        copies[i].start()
    notes = notes_ref[...]
    flag_ref[0] = jnp.max(notes[:, notes.shape[1] - 1 :]) + 1
    told = pltpu.make_async_copy(flag_ref, full_ref, sems.at[5])
    told.start()
    for copy in copies + [kept, told]:
        copy.wait()


PARAMS = pltpu.CompilerParams(vmem_limit_bytes=12 << 20)
VMEM = pl.BlockSpec(memory_space=pltpu.VMEM)
HBM = pl.BlockSpec(memory_space=pltpu.HBM)
SMEM = pl.BlockSpec(memory_space=pltpu.SMEM)
ANY = pl.BlockSpec(memory_space=pl.ANY)


def exchange(x, axis, groups):
    return lax.all_to_all(
        x, axis, split_axis=0, concat_axis=0, tiled=True, axis_index_groups=groups
    )


def pipeline(
    room,
    flux,
    patch_pft,
    patch_wt,
    patch_col,
    col_wt,
    col_lu,
    lu_wt,
    lu_grid,
    cell_target,
    patch_count,
    pft_scale,
    cpl_frac,
    cpl_field,
):
    devices = lax.axis_size("clump") * lax.axis_size("grp")
    patches, width = flux.shape[1:]
    cells = cell_target.shape[1]
    shape = jax.ShapeDtypeStruct
    lanes = 2 * width
    place = devices // PLANES
    columns = lax.axis_size("clump") // PLANES
    along = [[z * columns + i for z in range(PLANES)] for i in range(columns)]
    across = [[z * place + i for i in range(place)] for z in range(PLANES)]
    send, table, scaled, cell_of, first, second = pl.pallas_call(
        functools.partial(gather_kernel, devices),
        out_shape=(
            shape((PLANES * (room + 1), lanes), F32),
            shape((width + 1, cells), F32),
            shape((width, patches), F32),
            shape((cells, patches), BF16),
            shape((PLANES * room, cells), BF16),
            shape((PLANES * room, cells), BF16),
        ),
        in_specs=[SMEM] + [HBM] * 12,
        out_specs=(VMEM,) * 6,
        scratch_shapes=[
            pltpu.VMEM(col_lu.shape, jnp.int32),
            pltpu.VMEM(lu_wt.shape, F32),
            pltpu.VMEM(lu_grid.shape, jnp.int32),
            pltpu.VMEM(col_wt.shape, F32),
            pltpu.VMEM(patch_col.shape, jnp.int32),
            pltpu.VMEM(patch_pft.shape, jnp.int32),
            pltpu.VMEM(pft_scale.shape, F32),
            pltpu.VMEM(patch_wt.shape, F32),
            pltpu.VMEM(cell_target.shape, jnp.int32),
            pltpu.VMEM((width, patches), F32),
            pltpu.SemaphoreType.DMA((12,)),
        ],
        compiler_params=PARAMS,
        name="gather_cells",
    )(
        patch_count,
        *(
            pltpu.with_memory_space_constraint(x, pltpu.HBM)
            for x in (
                flux[0].T,
                patch_pft,
                patch_wt,
                patch_col,
                col_wt,
                col_lu,
                lu_wt,
                lu_grid,
                cell_target,
                pft_scale,
                cpl_field.T,
                cpl_frac.reshape(1, cells),
            )
        ),
    )
    noted = exchange(send.reshape(PLANES, 1, (room + 1) * lanes), "clump", along)
    noted = noted.reshape(PLANES * (room + 1), lanes)
    send = pl.pallas_call(
        turn_kernel,
        out_shape=shape((place * (PLANES + 1), lanes), F32),
        in_specs=[VMEM],
        out_specs=VMEM,
        compiler_params=PARAMS,
        name="turn_rows",
    )(noted)
    got = exchange(send.reshape(place, 1, (PLANES + 1) * lanes), AXES, across)
    mine, reply, notes = pl.pallas_call(
        merge_kernel,
        out_shape=(
            shape((width, cells), F32),
            shape((devices, lanes), F32),
            shape((8, lanes), jnp.int32),
        ),
        in_specs=[VMEM] * 2,
        out_specs=(VMEM, VMEM, VMEM),
        compiler_params=PARAMS,
        name="merge_cells",
    )(got.reshape(place * (PLANES + 1), lanes), table)
    back = exchange(reply.reshape(place, 1, PLANES * lanes), AXES, across)
    back = pl.pallas_call(
        turn_back_kernel,
        out_shape=shape((PLANES * room, lanes), F32),
        in_specs=[VMEM] * 2,
        out_specs=VMEM,
        compiler_params=PARAMS,
        name="turn_back",
    )(noted, back.reshape(devices, lanes))
    back = exchange(back.reshape(PLANES, 1, room * lanes), "clump", along)
    back = back.reshape(PLANES * room, lanes)
    anomaly, merged, full = pl.pallas_call(
        spread_kernel,
        out_shape=(
            shape((width, patches), F32),
            shape((width, cells), F32),
            shape((1,), jnp.int32),
        ),
        in_specs=[VMEM] * 7,
        out_specs=(ANY, ANY, ANY),
        scratch_shapes=[
            pltpu.VMEM((width, patches), F32),
            pltpu.SMEM((1,), jnp.int32),
            pltpu.SemaphoreType.DMA((6,)),
        ],
        compiler_params=PARAMS,
        name="spread_cells",
    )(back, first, second, cell_of, scaled, mine, notes)
    return merged, anomaly, full[0]


def per_device(*args):
    devices = lax.axis_size("clump") * lax.axis_size("grp")
    most = devices // PLANES

    def again(state):
        merged, anomaly, _ = pipeline(most, *args)
        return merged, anomaly, jnp.int32(0)

    merged, anomaly, _ = lax.while_loop(
        lambda state: state[2] > 0, again, pipeline(most // 2, *args)
    )
    return merged.T, anomaly.T[None]


def solution(mesh):
    rows = P(AXES, None)
    return jax.shard_map(
        per_device,
        mesh=mesh,
        in_specs=(
            P(AXES, None, None),
            rows,
            rows,
            rows,
            rows,
            rows,
            rows,
            rows,
            rows,
            P(AXES),
            P(),
            P(AXES),
            rows,
        ),
        out_specs=(rows, P(AXES, None, None)),
        check_vma=False,
    )
```

```python
import functools

import jax
import jax.numpy as jnp
from jax import lax
from jax.experimental import pallas as pl
from jax.experimental.pallas import tpu as pltpu
from jax.sharding import PartitionSpec as P

F32 = jnp.float32
BF16 = jnp.bfloat16
AXES = ("clump", "grp")
PLANES = 16


def pieces(x, count):
    parts = []
    for _ in range(count):
        part = x.astype(BF16)
        parts.append(part)
        x = x - part.astype(F32)
    return parts


def contract(a, b, da, db):
    return lax.dot_general(a, b, (((da,), (db,)), ((), ())), preferred_element_type=F32)


def onehot(mask):
    return jnp.where(mask, F32(1.0), F32(0.0)).astype(BF16)


def iota(shape, dim):
    return lax.broadcasted_iota(jnp.int32, shape, dim)


def cell_rows(target, cells, devices):
    place = devices // PLANES
    owner = target // cells
    across = jnp.broadcast_to(owner, (cells, cells)).astype(F32)
    down = across.T
    base = jnp.broadcast_to(owner - owner % place, (cells, cells)).astype(F32)
    earlier = (down == across) & (iota((cells, cells), 0) < iota((cells, cells), 1))
    rank = jnp.max(jnp.where(earlier, F32(1.0), F32(0.0)), axis=0, keepdims=True)
    below = (down < across) & (down >= base)
    row = jnp.sum(jnp.where(below, F32(0.5), F32(0.0)), axis=0, keepdims=True)
    return owner // place, owner % place, rank > 0.5, row.astype(jnp.int32)


def side_by_side(x):
    hi, lo = pieces(x, 2)
    both = jnp.concatenate([hi, lo], axis=1)
    zero = jnp.zeros_like(both)
    return jnp.concatenate(
        [jnp.concatenate([both, zero], axis=1), jnp.concatenate([zero, both], axis=1)], axis=0
    )


def from_rows(rows, first, second):
    width = rows.shape[1] // 2
    hi = rows.astype(BF16).astype(F32)
    lo = rows - hi
    left = iota(rows.shape, 1) < width
    one = jnp.where(left, hi, pltpu.roll(lo, width, 1)).astype(BF16)
    two = jnp.where(left, pltpu.roll(hi, width, 1), lo).astype(BF16)
    both = contract(
        jnp.concatenate([one, two], axis=0), jnp.concatenate([first, second], axis=0), 0, 0
    )
    return both[:width] + both[width:]


def gather_kernel(
    devices,
    count_ref,
    flux_ref,
    pft_ref,
    wt_ref,
    col_ref,
    col_wt_ref,
    col_lu_ref,
    lu_wt_ref,
    lu_grid_ref,
    target_ref,
    scale_ref,
    field_ref,
    frac_ref,
    send_ref,
    table_ref,
    scaled_ref,
    cell_of_ref,
    first_ref,
    second_ref,
    *scratch,
):
    held, sems = scratch[:-1], scratch[-1]
    given = (
        col_lu_ref,
        lu_wt_ref,
        lu_grid_ref,
        col_wt_ref,
        col_ref,
        pft_ref,
        scale_ref,
        wt_ref,
        target_ref,
        flux_ref,
    )
    copies = [
        pltpu.make_async_copy(src, dst, sems.at[i]) for i, (src, dst) in enumerate(zip(given, held))
    ]
    tables = [
        pltpu.make_async_copy(field_ref, table_ref.at[pl.ds(0, field_ref.shape[0])], sems.at[10]),
        pltpu.make_async_copy(frac_ref, table_ref.at[pl.ds(field_ref.shape[0], 1)], sems.at[11]),
    ]
    for copy in copies + tables:
        copy.start()
    (
        col_lu_ref,
        lu_wt_ref,
        lu_grid_ref,
        col_wt_ref,
        col_ref,
        pft_ref,
        scale_ref,
        wt_ref,
        target_ref,
        flux_ref,
    ) = held
    for copy in copies[:9]:
        copy.wait()
    width, patches = flux_ref.shape
    cells = target_ref.shape[1]
    room = send_ref.shape[0] // PLANES - 1
    lanes = send_ref.shape[1]
    columns = col_wt_ref.shape[1]
    units = lu_wt_ref.shape[1]
    types = scale_ref.shape[0]

    unit_table = jnp.concatenate(
        pieces(lu_wt_ref[...], 3)
        + [lu_grid_ref[...].astype(F32).astype(BF16), jnp.zeros((12, units), BF16)],
        axis=0,
    )
    unit_of = onehot(iota((units, columns), 0) == col_lu_ref[...])
    picked = contract(unit_table, unit_of, 1, 0)
    col_weight = col_wt_ref[...] * (picked[0:1] + picked[1:2] + picked[2:3])
    col_table = jnp.concatenate(
        pieces(col_weight, 3) + [picked[3:4].astype(BF16), jnp.zeros((12, columns), BF16)], axis=0
    )
    parts = []
    span = patches // 4
    for block in range(4):
        start = block * span
        low = max(start // 4, start - columns) // 128 * 128
        high = min(start + span, columns // 2 + start // 4 + span // 4, columns)
        high = -(-high // 128) * 128
        here = iota((high - low, span), 0) + low == col_ref[:, start : start + span]
        parts.append(contract(col_table[:, low:high], onehot(here), 1, 0))
    picked = jnp.concatenate(parts, axis=1)
    alive = iota((1, patches), 1) < count_ref[0]
    weight = jnp.where(
        alive, wt_ref[...] * (picked[0:1] + picked[1:2] + picked[2:3]), F32(0.0)
    )
    home = picked[3:4].astype(jnp.int32)

    type_of = onehot(iota((types, patches), 0) == pft_ref[...])
    scale_parts = jnp.concatenate(pieces(scale_ref[...], 3), axis=0)
    factor = contract(scale_parts, jnp.concatenate([type_of] * 3, axis=0), 0, 0)
    copies[9].wait()
    scaled = flux_ref[...] * factor
    scaled_ref[...] = jnp.where(alive, scaled, F32(0.0))

    cell_of = onehot((iota((cells, patches), 0) == home) & alive)
    cell_of_ref[...] = cell_of
    terms = jnp.concatenate([scaled * weight, weight, jnp.zeros((15, patches), F32)], axis=0)
    sums = [contract(part, cell_of, 1, 1) for part in pieces(terms, 2)]
    total = sums[0] + sums[1]
    mean = total[:width] / jnp.maximum(total[width : width + 1], 1.0)

    target = target_ref[...]
    plane, place, second, row = cell_rows(target, cells, devices)
    hit = iota((PLANES * room, cells), 0) == plane * room + row
    one, two = onehot(hit & jnp.logical_not(second)), onehot(hit & second)
    first_ref[...] = one
    second_ref[...] = two
    rows = contract(jnp.concatenate([one, one, two, two], axis=1), side_by_side(mean), 1, 1)

    in_plane = iota((PLANES, cells), 0) == plane
    slot = (target % cells + 1).astype(F32)
    seat = jnp.where(second, F32(0.0), (place + 1).astype(F32))
    left = jnp.concatenate(
        [jnp.where(in_plane, seat, F32(0.0)), jnp.where(in_plane, slot, F32(0.0))], axis=1
    ).astype(BF16)
    lane = iota((lanes, cells), 0)
    right = jnp.concatenate(
        [onehot(lane == row), onehot(lane == row + jnp.where(second, 2 * room, room))], axis=1
    )
    notes = contract(left, right, 1, 1)
    full = jnp.where(jnp.max(row, axis=1, keepdims=True) < room, F32(0.0), F32(1.0))
    notes = jnp.where(iota((PLANES, lanes), 1) == lanes - 1, full, notes)
    for z in range(PLANES):
        send_ref[pl.ds(z * (room + 1), room), :] = rows[z * room : (z + 1) * room]
    send_ref[pl.ds(room, PLANES, room + 1), :] = notes
    for copy in tables:
        copy.wait()


def seats(notes, z, place, room):
    return onehot(iota((place, room), 0) == notes[z : z + 1, :room].astype(jnp.int32) - 1)


def turn_kernel(got_ref, send_ref):
    room = got_ref.shape[0] // PLANES - 1
    place = send_ref.shape[0] // (PLANES + 1)
    lanes = got_ref.shape[1]
    notes = got_ref[pl.ds(room, PLANES, room + 1), :]
    turned = jnp.concatenate([notes, jnp.zeros((lanes - PLANES, lanes), F32)], axis=0).T
    slots = turned[room : 2 * room] + pltpu.roll(turned[2 * room : 3 * room], PLANES, 1)
    lane = iota((room, lanes), 1)
    picks, parts = [], []
    for z in range(PLANES):
        pick = seats(notes, z, place, room)
        hi, lo = pieces(got_ref[pl.ds(z * (room + 1), room), :], 2)
        send_ref[pl.ds(z, place, PLANES + 1), :] = contract(
            jnp.concatenate([pick, pick], axis=1), jnp.concatenate([hi, lo], axis=0), 1, 0
        )
        picks.append(pick)
        mine = (lane == z) | (lane == PLANES + z)
        parts.append(jnp.where(mine, slots, F32(0.0)).astype(BF16))
    passed = contract(jnp.concatenate(picks, axis=1), jnp.concatenate(parts, axis=0), 1, 0)
    full = jnp.max(notes[:, lanes - 1 :], axis=0, keepdims=True)
    passed = jnp.where(iota((place, lanes), 1) == lanes - 1, full, passed)
    send_ref[pl.ds(PLANES, place, PLANES + 1), :] = passed


def turn_back_kernel(got_ref, back_ref, send_ref):
    room = got_ref.shape[0] // PLANES - 1
    place = back_ref.shape[0] // PLANES
    notes = got_ref[pl.ds(room, PLANES, room + 1), :]
    for z in range(PLANES):
        pick = seats(notes, z, place, room)
        hi, lo = pieces(back_ref[pl.ds(z, place, PLANES), :], 2)
        send_ref[pl.ds(z * room, room), :] = contract(
            jnp.concatenate([pick, pick], axis=0), jnp.concatenate([hi, lo], axis=0), 0, 0
        )


def merge_kernel(got_ref, table_ref, merged_ref, reply_ref, full_ref):
    width, cells = merged_ref.shape
    devices = reply_ref.shape[0]
    place = devices // PLANES
    rows = jnp.concatenate(
        [got_ref[pl.ds(z, place, PLANES + 1), :] for z in range(PLANES)], axis=0
    )
    slots = got_ref[pl.ds(PLANES, place, PLANES + 1), :].astype(jnp.int32) - 1
    full_ref[...] = jnp.broadcast_to(jnp.max(slots, axis=0, keepdims=True), full_ref.shape)
    lane = iota((place, cells), 1)
    first, second = (
        jnp.concatenate(
            [onehot(lane == slots[:, k + z : k + z + 1]) for z in range(PLANES)], axis=0
        )
        for k in (0, PLANES)
    )
    field, frac = table_ref[:width, :], table_ref[width:, :]
    merged = frac * from_rows(rows, first, second) + (1.0 - frac) * field
    merged_ref[...] = merged
    masks = jnp.concatenate([first, first, second, second], axis=1)
    rows = contract(masks, side_by_side(merged), 1, 1)
    for z in range(PLANES):
        reply_ref[pl.ds(z, place, PLANES), :] = rows[z * place : (z + 1) * place]


def spread_kernel(
    back_ref,
    first_ref,
    second_ref,
    cell_of_ref,
    scaled_ref,
    mine_ref,
    notes_ref,
    out_ref,
    merged_ref,
    full_ref,
    held_ref,
    flag_ref,
    sems,
):
    width, patches = scaled_ref.shape
    kept = pltpu.make_async_copy(mine_ref, merged_ref, sems.at[4])
    kept.start()
    merged = from_rows(back_ref[...], first_ref[...], second_ref[...])
    both = jnp.concatenate(pieces(merged, 2), axis=0)
    chunk = patches // 4
    copies = []
    for i in range(4):
        here = pl.ds(i * chunk, chunk)
        parts = contract(both, cell_of_ref[:, here], 1, 0)
        held_ref[:, here] = scaled_ref[:, here] - (parts[:width] + parts[width:])
        copies.append(
            pltpu.make_async_copy(held_ref.at[:, here], out_ref.at[:, here], sems.at[i])
        )
        copies[i].start()
    notes = notes_ref[...]
    flag_ref[0] = jnp.max(notes[:, notes.shape[1] - 1 :]) + 1
    told = pltpu.make_async_copy(flag_ref, full_ref, sems.at[5])
    told.start()
    for copy in copies + [kept, told]:
        copy.wait()


PARAMS = pltpu.CompilerParams(vmem_limit_bytes=12 << 20)
VMEM = pl.BlockSpec(memory_space=pltpu.VMEM)
HBM = pl.BlockSpec(memory_space=pltpu.HBM)
SMEM = pl.BlockSpec(memory_space=pltpu.SMEM)
ANY = pl.BlockSpec(memory_space=pl.ANY)


def exchange(x, axis, groups):
    return lax.all_to_all(
        x, axis, split_axis=0, concat_axis=0, tiled=True, axis_index_groups=groups
    )


def pipeline(
    room,
    flux,
    patch_pft,
    patch_wt,
    patch_col,
    col_wt,
    col_lu,
    lu_wt,
    lu_grid,
    cell_target,
    patch_count,
    pft_scale,
    cpl_frac,
    cpl_field,
):
    devices = lax.axis_size("clump") * lax.axis_size("grp")
    patches, width = flux.shape[1:]
    cells = cell_target.shape[1]
    shape = jax.ShapeDtypeStruct
    lanes = 2 * width
    place = devices // PLANES
    columns = lax.axis_size("clump") // PLANES
    along = [[z * columns + i for z in range(PLANES)] for i in range(columns)]
    across = [[z * place + i for i in range(place)] for z in range(PLANES)]
    send, table, scaled, cell_of, first, second = pl.pallas_call(
        functools.partial(gather_kernel, devices),
        out_shape=(
            shape((PLANES * (room + 1), lanes), F32),
            shape((width + 1, cells), F32),
            shape((width, patches), F32),
            shape((cells, patches), BF16),
            shape((PLANES * room, cells), BF16),
            shape((PLANES * room, cells), BF16),
        ),
        in_specs=[SMEM] + [HBM] * 12,
        out_specs=(VMEM,) * 6,
        scratch_shapes=[
            pltpu.VMEM(col_lu.shape, jnp.int32),
            pltpu.VMEM(lu_wt.shape, F32),
            pltpu.VMEM(lu_grid.shape, jnp.int32),
            pltpu.VMEM(col_wt.shape, F32),
            pltpu.VMEM(patch_col.shape, jnp.int32),
            pltpu.VMEM(patch_pft.shape, jnp.int32),
            pltpu.VMEM(pft_scale.shape, F32),
            pltpu.VMEM(patch_wt.shape, F32),
            pltpu.VMEM(cell_target.shape, jnp.int32),
            pltpu.VMEM((width, patches), F32),
            pltpu.SemaphoreType.DMA((12,)),
        ],
        compiler_params=PARAMS,
        name="gather_cells",
    )(
        patch_count,
        *(
            pltpu.with_memory_space_constraint(x, pltpu.HBM)
            for x in (
                flux[0].T,
                patch_pft,
                patch_wt,
                patch_col,
                col_wt,
                col_lu,
                lu_wt,
                lu_grid,
                cell_target,
                pft_scale,
                cpl_field.T,
                cpl_frac.reshape(1, cells),
            )
        ),
    )
    noted = exchange(send.reshape(PLANES, 1, (room + 1) * lanes), "clump", along)
    noted = noted.reshape(PLANES * (room + 1), lanes)
    send = pl.pallas_call(
        turn_kernel,
        out_shape=shape((place * (PLANES + 1), lanes), F32),
        in_specs=[VMEM],
        out_specs=VMEM,
        compiler_params=PARAMS,
        name="turn_rows",
    )(noted)
    got = exchange(send.reshape(place, 1, (PLANES + 1) * lanes), AXES, across)
    mine, reply, notes = pl.pallas_call(
        merge_kernel,
        out_shape=(
            shape((width, cells), F32),
            shape((devices, lanes), F32),
            shape((8, lanes), jnp.int32),
        ),
        in_specs=[VMEM] * 2,
        out_specs=(VMEM, VMEM, VMEM),
        compiler_params=PARAMS,
        name="merge_cells",
    )(got.reshape(place * (PLANES + 1), lanes), table)
    back = exchange(reply.reshape(place, 1, PLANES * lanes), AXES, across)
    back = pl.pallas_call(
        turn_back_kernel,
        out_shape=shape((PLANES * room, lanes), F32),
        in_specs=[VMEM] * 2,
        out_specs=VMEM,
        compiler_params=PARAMS,
        name="turn_back",
    )(noted, back.reshape(devices, lanes))
    back = exchange(back.reshape(PLANES, 1, room * lanes), "clump", along)
    back = back.reshape(PLANES * room, lanes)
    anomaly, merged, full = pl.pallas_call(
        spread_kernel,
        out_shape=(
            shape((width, patches), F32),
            shape((width, cells), F32),
            shape((1,), jnp.int32),
        ),
        in_specs=[VMEM] * 7,
        out_specs=(ANY, ANY, ANY),
        scratch_shapes=[
            pltpu.VMEM((width, patches), F32),
            pltpu.SMEM((1,), jnp.int32),
            pltpu.SemaphoreType.DMA((6,)),
        ],
        compiler_params=PARAMS,
        name="spread_cells",
    )(back, first, second, cell_of, scaled, mine, notes)
    return merged, anomaly, full[0]


def per_device(*args):
    devices = lax.axis_size("clump") * lax.axis_size("grp")
    most = devices // PLANES

    def again(state):
        merged, anomaly, _ = pipeline(most, *args)
        return merged, anomaly, jnp.int32(0)

    merged, anomaly, _ = lax.while_loop(
        lambda state: state[2] > 0, again, pipeline(most * 15 // 32, *args)
    )
    return merged.T, anomaly.T[None]


def solution(mesh):
    rows = P(AXES, None)
    return jax.shard_map(
        per_device,
        mesh=mesh,
        in_specs=(
            P(AXES, None, None),
            rows,
            rows,
            rows,
            rows,
            rows,
            rows,
            rows,
            rows,
            P(AXES),
            P(),
            P(AXES),
            rows,
        ),
        out_specs=(rows, P(AXES, None, None)),
        check_vma=False,
    )
```

```python
import functools

import jax
import jax.numpy as jnp
from jax import lax
from jax.experimental import pallas as pl
from jax.experimental.pallas import tpu as pltpu
from jax.sharding import PartitionSpec as P

F32 = jnp.float32
BF16 = jnp.bfloat16
AXES = ("clump", "grp")
PLANES = 16


def pieces(x, count):
    parts = []
    for _ in range(count):
        part = x.astype(BF16)
        parts.append(part)
        x = x - part.astype(F32)
    return parts


def contract(a, b, da, db):
    return lax.dot_general(a, b, (((da,), (db,)), ((), ())), preferred_element_type=F32)


def onehot(mask):
    return jnp.where(mask, F32(1.0), F32(0.0)).astype(BF16)


def iota(shape, dim):
    return lax.broadcasted_iota(jnp.int32, shape, dim)


def cell_rows(target, cells, devices):
    place = devices // PLANES
    owner = target // cells
    across = jnp.broadcast_to(owner, (cells, cells)).astype(F32)
    down = across.T
    base = jnp.broadcast_to(owner - owner % place, (cells, cells)).astype(F32)
    earlier = (down == across) & (iota((cells, cells), 0) < iota((cells, cells), 1))
    rank = jnp.max(jnp.where(earlier, F32(1.0), F32(0.0)), axis=0, keepdims=True)
    below = (down < across) & (down >= base)
    row = jnp.sum(jnp.where(below, F32(0.5), F32(0.0)), axis=0, keepdims=True)
    return owner // place, owner % place, rank > 0.5, row.astype(jnp.int32)


def side_by_side(x):
    hi, lo = pieces(x, 2)
    both = jnp.concatenate([hi, lo], axis=1)
    zero = jnp.zeros_like(both)
    return jnp.concatenate(
        [jnp.concatenate([both, zero], axis=1), jnp.concatenate([zero, both], axis=1)], axis=0
    )


def from_rows(rows, first, second):
    width = rows.shape[1] // 2
    hi = rows.astype(BF16).astype(F32)
    lo = rows - hi
    left = iota(rows.shape, 1) < width
    one = jnp.where(left, hi, pltpu.roll(lo, width, 1)).astype(BF16)
    two = jnp.where(left, pltpu.roll(hi, width, 1), lo).astype(BF16)
    both = contract(
        jnp.concatenate([one, two], axis=0), jnp.concatenate([first, second], axis=0), 0, 0
    )
    return both[:width] + both[width:]


def gather_kernel(
    devices,
    count_ref,
    flux_ref,
    pft_ref,
    wt_ref,
    col_ref,
    col_wt_ref,
    col_lu_ref,
    lu_wt_ref,
    lu_grid_ref,
    target_ref,
    scale_ref,
    field_ref,
    frac_ref,
    send_ref,
    table_ref,
    scaled_ref,
    cell_of_ref,
    first_ref,
    second_ref,
    *scratch,
):
    held, sems = scratch[:-1], scratch[-1]
    given = (
        col_lu_ref,
        lu_wt_ref,
        lu_grid_ref,
        col_wt_ref,
        col_ref,
        pft_ref,
        scale_ref,
        wt_ref,
        target_ref,
        flux_ref,
    )
    copies = [
        pltpu.make_async_copy(src, dst, sems.at[i]) for i, (src, dst) in enumerate(zip(given, held))
    ]
    tables = [
        pltpu.make_async_copy(field_ref, table_ref.at[pl.ds(0, field_ref.shape[0])], sems.at[10]),
        pltpu.make_async_copy(frac_ref, table_ref.at[pl.ds(field_ref.shape[0], 1)], sems.at[11]),
    ]
    for copy in copies + tables:
        copy.start()
    (
        col_lu_ref,
        lu_wt_ref,
        lu_grid_ref,
        col_wt_ref,
        col_ref,
        pft_ref,
        scale_ref,
        wt_ref,
        target_ref,
        flux_ref,
    ) = held
    for copy in copies[:9]:
        copy.wait()
    width, patches = flux_ref.shape
    cells = target_ref.shape[1]
    room = send_ref.shape[0] // PLANES - 1
    lanes = send_ref.shape[1]
    columns = col_wt_ref.shape[1]
    units = lu_wt_ref.shape[1]
    types = scale_ref.shape[0]

    unit_table = jnp.concatenate(
        pieces(lu_wt_ref[...], 3)
        + [lu_grid_ref[...].astype(F32).astype(BF16), jnp.zeros((12, units), BF16)],
        axis=0,
    )
    unit_of = onehot(iota((units, columns), 0) == col_lu_ref[...])
    picked = contract(unit_table, unit_of, 1, 0)
    col_weight = col_wt_ref[...] * (picked[0:1] + picked[1:2] + picked[2:3])
    col_table = jnp.concatenate(
        pieces(col_weight, 3) + [picked[3:4].astype(BF16), jnp.zeros((12, columns), BF16)], axis=0
    )
    parts = []
    span = patches // 4
    for block in range(4):
        start = block * span
        low = max(start // 4, start - columns) // 128 * 128
        high = min(start + span, columns // 2 + start // 4 + span // 4, columns)
        high = -(-high // 128) * 128
        here = iota((high - low, span), 0) + low == col_ref[:, start : start + span]
        parts.append(contract(col_table[:, low:high], onehot(here), 1, 0))
    picked = jnp.concatenate(parts, axis=1)
    alive = iota((1, patches), 1) < count_ref[0]
    weight = jnp.where(
        alive, wt_ref[...] * (picked[0:1] + picked[1:2] + picked[2:3]), F32(0.0)
    )
    home = picked[3:4].astype(jnp.int32)

    type_of = onehot(iota((types, patches), 0) == pft_ref[...])
    scale_parts = jnp.concatenate(pieces(scale_ref[...], 3), axis=0)
    factor = contract(scale_parts, jnp.concatenate([type_of] * 3, axis=0), 0, 0)
    copies[9].wait()
    scaled = flux_ref[...] * factor
    scaled_ref[...] = jnp.where(alive, scaled, F32(0.0))

    cell_of = onehot((iota((cells, patches), 0) == home) & alive)
    cell_of_ref[...] = cell_of
    terms = jnp.concatenate([scaled * weight, weight, jnp.zeros((15, patches), F32)], axis=0)
    sums = [contract(part, cell_of, 1, 1) for part in pieces(terms, 2)]
    total = sums[0] + sums[1]
    mean = total[:width] / jnp.maximum(total[width : width + 1], 1.0)

    target = target_ref[...]
    plane, place, second, row = cell_rows(target, cells, devices)
    hit = iota((PLANES * room, cells), 0) == plane * room + row
    one, two = onehot(hit & jnp.logical_not(second)), onehot(hit & second)
    first_ref[...] = one
    second_ref[...] = two
    rows = contract(jnp.concatenate([one, one, two, two], axis=1), side_by_side(mean), 1, 1)

    in_plane = iota((PLANES, cells), 0) == plane
    slot = (target % cells + 1).astype(F32)
    seat = jnp.where(second, F32(0.0), (place + 1).astype(F32))
    left = jnp.concatenate(
        [jnp.where(in_plane, seat, F32(0.0)), jnp.where(in_plane, slot, F32(0.0))], axis=1
    ).astype(BF16)
    lane = iota((lanes, cells), 0)
    right = jnp.concatenate(
        [onehot(lane == row), onehot(lane == row + jnp.where(second, 2 * room, room))], axis=1
    )
    notes = contract(left, right, 1, 1)
    full = jnp.where(jnp.max(row, axis=1, keepdims=True) < room, F32(0.0), F32(1.0))
    notes = jnp.where(iota((PLANES, lanes), 1) == lanes - 1, full, notes)
    for z in range(PLANES):
        send_ref[pl.ds(z * (room + 1), room), :] = rows[z * room : (z + 1) * room]
    send_ref[pl.ds(room, PLANES, room + 1), :] = notes
    for copy in tables:
        copy.wait()


def seats(notes, z, place, room):
    return onehot(iota((place, room), 0) == notes[z : z + 1, :room].astype(jnp.int32) - 1)


def turn_kernel(got_ref, send_ref):
    room = got_ref.shape[0] // PLANES - 1
    place = send_ref.shape[0] // (PLANES + 1)
    lanes = got_ref.shape[1]
    notes = got_ref[pl.ds(room, PLANES, room + 1), :]
    turned = jnp.concatenate([notes, jnp.zeros((lanes - PLANES, lanes), F32)], axis=0).T
    slots = turned[room : 2 * room] + pltpu.roll(turned[2 * room : 3 * room], PLANES, 1)
    lane = iota((room, lanes), 1)
    picks, parts = [], []
    for z in range(PLANES):
        pick = seats(notes, z, place, room)
        hi, lo = pieces(got_ref[pl.ds(z * (room + 1), room), :], 2)
        send_ref[pl.ds(z, place, PLANES + 1), :] = contract(
            jnp.concatenate([pick, pick], axis=1), jnp.concatenate([hi, lo], axis=0), 1, 0
        )
        picks.append(pick)
        mine = (lane == z) | (lane == PLANES + z)
        parts.append(jnp.where(mine, slots, F32(0.0)).astype(BF16))
    passed = contract(jnp.concatenate(picks, axis=1), jnp.concatenate(parts, axis=0), 1, 0)
    full = jnp.max(notes[:, lanes - 1 :], axis=0, keepdims=True)
    passed = jnp.where(iota((place, lanes), 1) == lanes - 1, full, passed)
    send_ref[pl.ds(PLANES, place, PLANES + 1), :] = passed


def turn_back_kernel(got_ref, back_ref, send_ref):
    room = got_ref.shape[0] // PLANES - 1
    place = back_ref.shape[0] // PLANES
    notes = got_ref[pl.ds(room, PLANES, room + 1), :]
    for z in range(PLANES):
        pick = seats(notes, z, place, room)
        hi, lo = pieces(back_ref[pl.ds(z, place, PLANES), :], 2)
        send_ref[pl.ds(z * room, room), :] = contract(
            jnp.concatenate([pick, pick], axis=0), jnp.concatenate([hi, lo], axis=0), 0, 0
        )


def merge_kernel(got_ref, table_ref, merged_ref, reply_ref, full_ref):
    width, cells = merged_ref.shape
    devices = reply_ref.shape[0]
    place = devices // PLANES
    rows = jnp.concatenate(
        [got_ref[pl.ds(z, place, PLANES + 1), :] for z in range(PLANES)], axis=0
    )
    slots = got_ref[pl.ds(PLANES, place, PLANES + 1), :].astype(jnp.int32) - 1
    full_ref[...] = jnp.broadcast_to(jnp.max(slots, axis=0, keepdims=True), full_ref.shape)
    lane = iota((place, cells), 1)
    first, second = (
        jnp.concatenate(
            [onehot(lane == slots[:, k + z : k + z + 1]) for z in range(PLANES)], axis=0
        )
        for k in (0, PLANES)
    )
    field, frac = table_ref[:width, :], table_ref[width:, :]
    merged = frac * from_rows(rows, first, second) + (1.0 - frac) * field
    merged_ref[...] = merged
    masks = jnp.concatenate([first, first, second, second], axis=1)
    rows = contract(masks, side_by_side(merged), 1, 1)
    for z in range(PLANES):
        reply_ref[pl.ds(z, place, PLANES), :] = rows[z * place : (z + 1) * place]


def spread_kernel(
    back_ref,
    first_ref,
    second_ref,
    cell_of_ref,
    scaled_ref,
    mine_ref,
    notes_ref,
    out_ref,
    merged_ref,
    full_ref,
    held_ref,
    flag_ref,
    sems,
):
    width, patches = scaled_ref.shape
    kept = pltpu.make_async_copy(mine_ref, merged_ref, sems.at[4])
    kept.start()
    merged = from_rows(back_ref[...], first_ref[...], second_ref[...])
    both = jnp.concatenate(pieces(merged, 2), axis=0)
    chunk = patches // 4
    copies = []
    for i in range(4):
        here = pl.ds(i * chunk, chunk)
        parts = contract(both, cell_of_ref[:, here], 1, 0)
        held_ref[:, here] = scaled_ref[:, here] - (parts[:width] + parts[width:])
        copies.append(
            pltpu.make_async_copy(held_ref.at[:, here], out_ref.at[:, here], sems.at[i])
        )
        copies[i].start()
    notes = notes_ref[...]
    flag_ref[0] = jnp.max(notes[:, notes.shape[1] - 1 :]) + 1
    told = pltpu.make_async_copy(flag_ref, full_ref, sems.at[5])
    told.start()
    for copy in copies + [kept, told]:
        copy.wait()


PARAMS = pltpu.CompilerParams(vmem_limit_bytes=12 << 20)
VMEM = pl.BlockSpec(memory_space=pltpu.VMEM)
HBM = pl.BlockSpec(memory_space=pltpu.HBM)
SMEM = pl.BlockSpec(memory_space=pltpu.SMEM)
ANY = pl.BlockSpec(memory_space=pl.ANY)


def exchange(x, axis, groups):
    return lax.all_to_all(
        x, axis, split_axis=0, concat_axis=0, tiled=True, axis_index_groups=groups
    )


def pipeline(
    room,
    flux,
    patch_pft,
    patch_wt,
    patch_col,
    col_wt,
    col_lu,
    lu_wt,
    lu_grid,
    cell_target,
    patch_count,
    pft_scale,
    cpl_frac,
    cpl_field,
):
    devices = lax.axis_size("clump") * lax.axis_size("grp")
    patches, width = flux.shape[1:]
    cells = cell_target.shape[1]
    shape = jax.ShapeDtypeStruct
    lanes = 2 * width
    place = devices // PLANES
    columns = lax.axis_size("clump") // PLANES
    along = [[z * columns + i for z in range(PLANES)] for i in range(columns)]
    across = [[z * place + i for i in range(place)] for z in range(PLANES)]
    send, table, scaled, cell_of, first, second = pl.pallas_call(
        functools.partial(gather_kernel, devices),
        out_shape=(
            shape((PLANES * (room + 1), lanes), F32),
            shape((width + 1, cells), F32),
            shape((width, patches), F32),
            shape((cells, patches), BF16),
            shape((PLANES * room, cells), BF16),
            shape((PLANES * room, cells), BF16),
        ),
        in_specs=[SMEM] + [HBM] * 12,
        out_specs=(VMEM,) * 6,
        scratch_shapes=[
            pltpu.VMEM(col_lu.shape, jnp.int32),
            pltpu.VMEM(lu_wt.shape, F32),
            pltpu.VMEM(lu_grid.shape, jnp.int32),
            pltpu.VMEM(col_wt.shape, F32),
            pltpu.VMEM(patch_col.shape, jnp.int32),
            pltpu.VMEM(patch_pft.shape, jnp.int32),
            pltpu.VMEM(pft_scale.shape, F32),
            pltpu.VMEM(patch_wt.shape, F32),
            pltpu.VMEM(cell_target.shape, jnp.int32),
            pltpu.VMEM((width, patches), F32),
            pltpu.SemaphoreType.DMA((12,)),
        ],
        compiler_params=PARAMS,
        name="gather_cells",
    )(
        patch_count,
        *(
            pltpu.with_memory_space_constraint(x, pltpu.HBM)
            for x in (
                flux[0].T,
                patch_pft,
                patch_wt,
                patch_col,
                col_wt,
                col_lu,
                lu_wt,
                lu_grid,
                cell_target,
                pft_scale,
                cpl_field.T,
                cpl_frac.reshape(1, cells),
            )
        ),
    )
    noted = exchange(send.reshape(PLANES, 1, (room + 1) * lanes), "clump", along)
    noted = noted.reshape(PLANES * (room + 1), lanes)
    send = pl.pallas_call(
        turn_kernel,
        out_shape=shape((place * (PLANES + 1), lanes), F32),
        in_specs=[VMEM],
        out_specs=VMEM,
        compiler_params=PARAMS,
        name="turn_rows",
    )(noted)
    got = exchange(send.reshape(place, 1, (PLANES + 1) * lanes), AXES, across)
    mine, reply, notes = pl.pallas_call(
        merge_kernel,
        out_shape=(
            shape((width, cells), F32),
            shape((devices, lanes), F32),
            shape((8, lanes), jnp.int32),
        ),
        in_specs=[VMEM] * 2,
        out_specs=(VMEM, VMEM, VMEM),
        compiler_params=PARAMS,
        name="merge_cells",
    )(got.reshape(place * (PLANES + 1), lanes), table)
    back = exchange(reply.reshape(place, 1, PLANES * lanes), AXES, across)
    back = pl.pallas_call(
        turn_back_kernel,
        out_shape=shape((PLANES * room, lanes), F32),
        in_specs=[VMEM] * 2,
        out_specs=VMEM,
        compiler_params=PARAMS,
        name="turn_back",
    )(noted, back.reshape(devices, lanes))
    back = exchange(back.reshape(PLANES, 1, room * lanes), "clump", along)
    back = back.reshape(PLANES * room, lanes)
    anomaly, merged, full = pl.pallas_call(
        spread_kernel,
        out_shape=(
            shape((width, patches), F32),
            shape((width, cells), F32),
            shape((1,), jnp.int32),
        ),
        in_specs=[VMEM] * 7,
        out_specs=(ANY, ANY, ANY),
        scratch_shapes=[
            pltpu.VMEM((width, patches), F32),
            pltpu.SMEM((1,), jnp.int32),
            pltpu.SemaphoreType.DMA((6,)),
        ],
        compiler_params=PARAMS,
        name="spread_cells",
    )(back, first, second, cell_of, scaled, mine, notes)
    return merged, anomaly, full[0]


def per_device(*args):
    devices = lax.axis_size("clump") * lax.axis_size("grp")
    most = devices // PLANES

    merged, anomaly, full = pipeline(most * 15 // 32, *args)
    merged, anomaly, full, args = lax.optimization_barrier((merged, anomaly, full, args))
    merged, anomaly = lax.cond(
        full > 0,
        lambda held, given: pipeline(most, *given)[:2],
        lambda held, given: held,
        (merged, anomaly),
        args,
    )
    return merged.T, anomaly.T[None]


def solution(mesh):
    rows = P(AXES, None)
    return jax.shard_map(
        per_device,
        mesh=mesh,
        in_specs=(
            P(AXES, None, None),
            rows,
            rows,
            rows,
            rows,
            rows,
            rows,
            rows,
            rows,
            P(AXES),
            P(),
            P(AXES),
            rows,
        ),
        out_specs=(rows, P(AXES, None, None)),
        check_vma=False,
    )
```
